32 devices in a mesh: level: 4 (over x, core), tile: 8 (over z, y).
Axes of the slice: x: 2, y: 2, z: 4, core: 2. Of those that a mesh axis runs over, the one named last changes fastest.
Arguments:
- queue_init: bfloat16 [4, 4, 4, 32, 128], P('level', None, None, 'tile'), may hold values from -6 to 6
- noise_frames: bfloat16 [2, 4, 4, 32, 128], P(None, None, None, 'tile'), may hold values from -6 to 6
- conv_first: bfloat16 [3, 3, 320, 4], replicated, may hold values from -1 to 1
- conv_second: bfloat16 [3, 3, 320, 320], replicated, may hold values from -0.109375 to 0.109375
- time_weight: bfloat16 [3, 320, 320], replicated, may hold values from -0.1875 to 0.1875
- out_proj: bfloat16 [4, 320], replicated, may hold values from -0.3125 to 0.3125
- keep_coef: float32 [2, 4, 4], replicated, may hold values from 0.6 to 1
- noise_coef: float32 [2, 4, 4], replicated, may hold values from 0.1 to 0.5
Outputs:
- queue_final: bfloat16 [4, 4, 4, 32, 128], P('level', None, None, 'tile')
The draws below stay inside these ranges and needn't reach their ends.
All inputs are finite; a program needn't handle non-finite values.
Results may differ from the reference program's by a relative error of at most 0.0048.
Values may be sent and summed in bfloat16 or wider, within the bound.
No kernel may reach another device: no remote copies, remote signals or barrier semaphores. Data moves between devices by JAX's collectives and lax.ppermute only.
A program may use at most 64 MiB of HBM per device.

```python
import math
import jax
import jax.numpy as jnp
from jax import lax

CHANNELS = 320
LATENT = 4
FRAMES = 4
WIDTH = 128
STEPS = 2
GROUPS = 4
HEIGHT = 32


def block_levels(own_key, extent, pieces, low, largest):
    def one(position, shards_of):
        heights = jax.random.uniform(jax.random.fold_in(jax.random.fold_in(own_key, 6), position), (shards_of,), jnp.float32, low / len(pieces), largest / len(pieces))
        return jnp.repeat(jnp.exp(heights), extent[position] // shards_of).reshape((-1,) + (1,) * (len(extent) - position - 1))

    loudness = one(*pieces[0])
    for cut in pieces[1:]:
        loudness = loudness * one(*cut)
    return loudness


def centred(own_key, dims, scale, limit, pieces=(), held_as=jnp.bfloat16):
    gain = block_levels(own_key, dims, pieces, -0.22, 0.18) if pieces else 1.0
    array = jax.random.normal(own_key, dims, jnp.float32) * scale * gain
    return jnp.minimum(jnp.maximum(array, -limit), limit).astype(held_as)


def setup_inputs(seed: int = 0) -> dict:
    key_of = jax.random.split(jax.random.key(seed), 9)
    queue_init = centred(key_of[0], (GROUPS, FRAMES, LATENT, HEIGHT, WIDTH), 1.0, 6.0, ((0, 4), (3, 8)))
    noise_frames = centred(key_of[1], (STEPS, FRAMES, LATENT, HEIGHT, WIDTH), 1.0, 6.0, ((3, 8),))
    conv_first = centred(key_of[2], (3, 3, CHANNELS, LATENT), (9 * LATENT) ** -0.5, 1.0)
    conv_second = centred(key_of[3], (3, 3, CHANNELS, CHANNELS), (9 * CHANNELS) ** -0.5, 0.109375)
    time_weight = centred(key_of[4], (3, CHANNELS, CHANNELS), (3 * CHANNELS) ** -0.5, 0.1875)
    out_proj = centred(key_of[5], (LATENT, CHANNELS), CHANNELS ** -0.5, 0.3125)
    keep_coef = jnp.clip(jnp.exp(jax.random.uniform(key_of[6], (STEPS, GROUPS, FRAMES), jnp.float32, math.log(0.6), math.log(1.0))), 0.6, 1.0)
    noise_coef = jnp.clip(jnp.exp(jax.random.uniform(key_of[7], (STEPS, GROUPS, FRAMES), jnp.float32, math.log(0.1), math.log(0.5))), 0.1, 0.5)
    return dict(queue_init=queue_init, noise_frames=noise_frames, conv_first=conv_first, conv_second=conv_second, time_weight=time_weight, out_proj=out_proj, keep_coef=keep_coef, noise_coef=noise_coef)


def conv_frames(frames, weight):
    padded = jnp.pad(frames.astype(jnp.float32), ((0, 0), (0, 0), (1, 1), (1, 1)))
    weight_full = weight.astype(jnp.float32)
    height_now = frames.shape[2]
    width_now = frames.shape[3]
    running = jnp.zeros((frames.shape[0], weight.shape[2], height_now, width_now), jnp.float32)
    for row_tap in range(3):
        for col_tap in range(3):
            window = padded[:, :, row_tap:row_tap + height_now, col_tap:col_tap + width_now]
            running = running + jnp.einsum('oc,fchw->fohw', weight_full[row_tap, col_tap], window)
    return running


def reference(queue_init, noise_frames, conv_first, conv_second, time_weight, out_proj, keep_coef, noise_coef):
    queued = queue_init
    time_full = time_weight.astype(jnp.float32)
    proj_full = out_proj.astype(jnp.float32)
    for step_index in range(STEPS):
        queued = jnp.concatenate([noise_frames[step_index][None], queued[:-1]], axis=0)
        first_act = lax.map(lambda group: jax.nn.silu(conv_frames(group, conv_first)).astype(jnp.bfloat16), queued)
        second = lax.map(lambda group: conv_frames(group, conv_second), first_act)
        active = jax.nn.silu(second).astype(jnp.bfloat16)
        flat = active.reshape((GROUPS * FRAMES,) + active.shape[2:])
        padded = jnp.pad(flat, ((1, 1), (0, 0), (0, 0), (0, 0)))

        def temporal_group(group_index):
            window = lax.dynamic_slice_in_dim(padded, group_index * FRAMES, FRAMES + 2, 0).astype(jnp.float32)
            running = jnp.einsum('oc,fchw->fohw', time_full[0], window[0:FRAMES])
            running = running + jnp.einsum('oc,fchw->fohw', time_full[1], window[1:FRAMES + 1])
            running = running + jnp.einsum('oc,fchw->fohw', time_full[2], window[2:FRAMES + 2])
            return running

        temporal = lax.map(temporal_group, jnp.arange(GROUPS, dtype=jnp.int32))
        predicted = (second + temporal).astype(jnp.bfloat16)
        projected = lax.map(lambda group: jnp.einsum('oc,fchw->fohw', proj_full, group.astype(jnp.float32)), predicted)
        keep_rate = keep_coef[step_index][:, :, None, None, None]
        noise_rate = noise_coef[step_index][:, :, None, None, None]
        queued = (keep_rate * queued.astype(jnp.float32) - noise_rate * projected).astype(jnp.bfloat16)
    return queued
```

```python
import functools

import jax
import jax.numpy as jnp
from jax import lax
from jax.experimental import pallas as pl
from jax.experimental.pallas import tpu as pltpu
from jax.sharding import PartitionSpec as P

BF16 = jnp.bfloat16
F32 = jnp.float32


def silu(v):
    half = 0.5 * v
    return half * jnp.tanh(half) + half


def step_kernel(
    dims, edge_ref, keep_ref, noise_ref, prev_ref, own_ref, next_ref, w1_ref, w2_ref, wz_ref,
    upd_ref, fwd_ref, bwd_ref, s_ref, z_ref,
):
    frames, latent, rows, width, channels = dims
    n_out = rows * width
    n_mid = (rows + 2) * width
    n_in = (rows + 4) * width
    slot = w1_ref.shape[1] // 3

    def shift_cols(v, by):
        lane = lax.broadcasted_iota(jnp.int32, v.shape, 1) % width
        if by > 0:
            return jnp.where(lane == 0, jnp.zeros_like(v), pltpu.roll(v, 1, 1))
        return jnp.where(lane == width - 1, jnp.zeros_like(v), pltpu.roll(v, v.shape[1] - 1, 1))

    def conv1(f):
        lo, hi = f * latent, (f + 1) * latent
        a = jnp.concatenate(
            [prev_ref[lo:hi, :], own_ref[lo:hi, :], next_ref[lo:hi, :]], axis=1
        ).astype(F32)
        parts = [shift_cols(a, 1), a, shift_cols(a, -1)]
        if slot > 3 * latent:
            parts.append(jnp.zeros((slot - 3 * latent, n_in), F32))
        b = jnp.concatenate(parts, axis=0).astype(BF16)
        x = jnp.concatenate([b[:, k * width:k * width + n_mid] for k in range(3)], axis=0)
        v = silu(jnp.dot(w1_ref[...], x, preferred_element_type=F32))
        row = lax.broadcasted_iota(jnp.int32, v.shape, 1) // width
        outside = ((row == 0) & (edge_ref[0] == 1)) | ((row == rows + 1) & (edge_ref[1] == 1))
        v = jnp.where(outside, 0.0, v)
        s_ref[f % 2, 0:channels, :] = shift_cols(v, 1).astype(BF16)
        s_ref[f % 2, channels:2 * channels, :] = v.astype(BF16)
        s_ref[f % 2, 2 * channels:, :] = shift_cols(v, -1).astype(BF16)

    def conv2(f):
        total = None
        for k in range(3):
            part = jnp.dot(
                w2_ref[k], s_ref[f % 2, :, k * width:k * width + n_out],
                preferred_element_type=F32,
            )
            total = part if total is None else total + part
        return total

    def project(f, second):
        x = jnp.concatenate([second.astype(BF16), silu(second).astype(BF16)], axis=0)
        z_ref[f] = jnp.dot(wz_ref[...], x, preferred_element_type=F32)

    conv1(0)
    for f in range(frames):
        if f + 1 < frames:
            conv1(f + 1)
        project(f, conv2(f))
    for f in range(frames):
        z = z_ref[f, 0:latent, :]
        if f > 0:
            z = z + z_ref[f - 1, latent:2 * latent, :]
        if f + 1 < frames:
            z = z + z_ref[f + 1, 2 * latent:3 * latent, :]
        lo, hi = f * latent, (f + 1) * latent
        upd_ref[lo:hi, :] = keep_ref[f] * own_ref[lo:hi, :].astype(F32) - noise_ref[f] * z
    fwd_ref[...] = z_ref[frames - 1, latent:2 * latent, :]
    bwd_ref[...] = z_ref[0, 2 * latent:3 * latent, :]


def per_device(
    queue_init, noise_frames, conv_first, conv_second, time_weight, out_proj, keep_coef, noise_coef
):
    steps = noise_frames.shape[0]
    _, frames, latent, rows, width = queue_init.shape
    channels = conv_second.shape[2]
    levels, tiles = lax.axis_size("level"), lax.axis_size("tile")
    level, tile = lax.axis_index("level"), lax.axis_index("tile")
    flat = frames * latent
    n_out = rows * width
    dims = (frames, latent, rows, width, channels)
    half = 2 * width

    slot = -(-3 * latent // 16) * 16
    w1 = jnp.transpose(conv_first, (2, 0, 1, 3)).reshape(channels, 3, 3 * latent)
    w1 = jnp.pad(w1, ((0, 0), (0, 0), (0, slot - 3 * latent))).reshape(channels, 3 * slot)
    w2 = jnp.transpose(conv_second, (0, 2, 1, 3)).reshape(3, channels, 3 * channels)
    pt = jnp.einsum("lo,koi->kli", out_proj, time_weight, preferred_element_type=F32).astype(BF16)
    left = jnp.zeros((4 * latent, channels), BF16).at[0:latent].set(out_proj)
    right = jnp.concatenate([pt[1], pt[0], pt[2], jnp.zeros((latent, channels), BF16)], axis=0)
    wz = jnp.concatenate([left, right], axis=1)
    edge = jnp.stack([tile == 0, tile == tiles - 1]).astype(jnp.int32)

    def permute(x, dl, dt):
        pairs = [
            (l * tiles + t, ((l + dl) % levels) * tiles + t + dt)
            for l in range(levels) for t in range(tiles) if 0 <= t + dt < tiles
        ]
        return lax.ppermute(x, ("level", "tile"), pairs)

    def level_chain(x, by, skip):
        pairs = [(l, (l + by) % levels) for l in range(levels) if l != skip]
        return lax.ppermute(x, "level", pairs)

    queue = queue_init[0].reshape(flat, n_out)
    noise = noise_frames.reshape(steps, flat, n_out)
    send = jnp.where(level == levels - 1, noise[0], queue)
    own = permute(send, steps, 0)
    prev = permute(send[:, n_out - half:], steps, 1)
    nxt = permute(send[:, :half], steps, -1)

    smem = pl.BlockSpec(memory_space=pltpu.SMEM)
    vmem = pl.BlockSpec(memory_space=pltpu.VMEM)
    flops = 2 * frames * n_out * channels * (9 * channels + 9 * latent * 2 + 8 * latent)
    call = pl.pallas_call(
        functools.partial(step_kernel, dims),
        out_shape=(
            jax.ShapeDtypeStruct((flat, n_out), F32),
            jax.ShapeDtypeStruct((latent, n_out), F32),
            jax.ShapeDtypeStruct((latent, n_out), F32),
        ),
        in_specs=[smem] * 3 + [vmem] * 6,
        out_specs=(vmem,) * 3,
        scratch_shapes=[
            pltpu.VMEM((2, 3 * channels, (rows + 2) * width), BF16),
            pltpu.VMEM((frames, 4 * latent, n_out), F32),
        ],
        compiler_params=pltpu.CompilerParams(vmem_limit_bytes=32 * 1024 * 1024),
        cost_estimate=pl.CostEstimate(
            flops=flops, bytes_accessed=2 * 9 * channels * channels, transcendentals=0
        ),
    )

    for s in range(steps):
        offset = steps - 1 - s
        position = (level + levels - offset % levels) % levels
        keep = lax.dynamic_index_in_dim(keep_coef[s], position, 0, keepdims=False)
        rate = lax.dynamic_index_in_dim(noise_coef[s], position, 0, keepdims=False)
        upd, fwd, bwd = call(edge, keep, rate, prev, own, nxt, w1, w2, wz)
        last = (levels - 1 + offset) % levels
        before = level_chain(fwd, 1, last)
        after = level_chain(bwd, -1, (last + 1) % levels)
        gap = jnp.zeros((flat - 2 * latent, n_out), F32)
        corr = jnp.concatenate([rate[0] * before, gap, rate[frames - 1] * after], axis=0)
        queue = (upd - corr).astype(BF16)
        if s + 1 < steps:
            queue = jnp.where(position == levels - 1, noise[s + 1], queue)
            own = queue
            prev = permute(queue[:, n_out - half:], 0, 1)
            nxt = permute(queue[:, :half], 0, -1)
    return queue.reshape(1, frames, latent, rows, width)


def solution(mesh):
    return jax.shard_map(
        per_device,
        mesh=mesh,
        in_specs=(
            P("level", None, None, "tile", None),
            P(None, None, None, "tile", None),
            P(),
            P(),
            P(),
            P(),
            P(),
            P(),
        ),
        out_specs=P("level", None, None, "tile", None),
        check_vma=False,
    )
```

```python
import functools

import jax
import jax.numpy as jnp
from jax import lax
from jax.experimental import pallas as pl
from jax.experimental.pallas import tpu as pltpu
from jax.sharding import PartitionSpec as P

BF16 = jnp.bfloat16
F32 = jnp.float32
MIB = 1024 * 1024


def silu(v):
    half = 0.5 * v
    return half * jnp.tanh(half) + half


def dot(a, b):
    return jnp.dot(a, b, preferred_element_type=F32)


def slot_of(latent):
    return -(-3 * latent // 16) * 16


def lanes(n):
    return -(-n // 128) * 128


def prep_kernel(first_ref, second_ref, time_ref, proj_ref, w1_ref, w2_ref, wz_ref):
    taps, channels, latent = first_ref.shape
    slot = slot_of(latent)
    row = lax.broadcasted_iota(jnp.int32, (latent, w1_ref.shape[1]), 0)
    col = lax.broadcasted_iota(jnp.int32, (latent, w1_ref.shape[1]), 1)
    w1 = jnp.zeros(w1_ref.shape, F32)
    for tap in range(taps):
        base = tap // 3 * slot + tap % 3 * latent
        place = jnp.where(col == row + base, 1.0, 0.0).astype(BF16)
        w1 = w1 + dot(first_ref[tap], place)
    w1_ref[...] = w1.astype(BF16)
    for b in range(3):
        g = [second_ref[3 * a + b].astype(F32) for a in range(3)]
        outer = 0.5 * (g[0] + g[2])
        forms = [g[0], -outer - 0.5 * g[1], outer - 0.5 * g[1], -g[2]]
        for k in range(4):
            w2_ref[k, :, b * channels:(b + 1) * channels] = forms[k].astype(BF16)
    spare = w2_ref.shape[2] - 3 * channels
    if spare:
        w2_ref[:, :, 3 * channels:] = jnp.zeros((4, channels, spare), BF16)
    proj = proj_ref[...]
    zero = jnp.zeros((latent, channels), F32)
    pt = [dot(proj, time_ref[k]) for k in range(3)]
    left = jnp.concatenate([proj.astype(F32), zero, zero, zero], axis=0)
    right = jnp.concatenate([pt[1], pt[0], pt[2], zero], axis=0)
    wz_ref[:, 0:channels] = left.astype(BF16)
    wz_ref[:, channels:] = right.astype(BF16)


def convolve(batches, latents, dims, rows, tile, tiles, w1_ref, w2_ref, wz_ref, s_ref, store):
    latent, local_rows, width, channels = dims
    slot = slot_of(latent)
    pairs = rows // 2
    n_mid = (rows + 2) * width
    extra = (rows - local_rows) // 2
    span = pairs * width

    def shift_cols(v, by):
        lane = lax.broadcasted_iota(jnp.int32, v.shape, 1) % width
        if by > 0:
            return jnp.where(lane == 0, jnp.zeros_like(v), pltpu.roll(v, 1, 1))
        return jnp.where(lane == width - 1, jnp.zeros_like(v), pltpu.roll(v, v.shape[1] - 1, 1))

    def conv1(i, frames):
        for j, f in enumerate(frames):
            a = latents(f)
            parts = [shift_cols(a, 1), a, shift_cols(a, -1)]
            if slot > 3 * latent:
                parts.append(jnp.zeros((slot - 3 * latent, a.shape[1]), F32))
            b = jnp.concatenate(parts, axis=0).astype(BF16)
            x = jnp.concatenate([b[:, k * width:k * width + n_mid] for k in range(3)], axis=0)
            v = silu(dot(w1_ref[:, 0:3 * slot], x))
            row = lax.broadcasted_iota(jnp.int32, v.shape, 1) // width
            low = jnp.where(tile == 0, extra + 1, 0)
            high = jnp.where(tile == tiles - 1, extra + 1 + local_rows, rows + 2)
            v = jnp.where((row < low) | (row >= high), 0.0, v).astype(BF16).astype(F32)
            d = [v[:, k * width:(k + 1) * width] for k in range(rows + 2)]
            at = slice(j * span, (j + 1) * span)
            for k in range(4):
                forms = []
                for p in range(pairs):
                    e = d[2 * p:2 * p + 4]
                    forms.append((e[0] - e[2], e[1] + e[2], e[2] - e[1], e[1] - e[3])[k])
                form = jnp.concatenate(forms, axis=1) if pairs > 1 else forms[0]
                s_ref[i % 2, k, 0:channels, at] = shift_cols(form, 1).astype(BF16)
                s_ref[i % 2, k, channels:2 * channels, at] = form.astype(BF16)
                s_ref[i % 2, k, 2 * channels:, at] = shift_cols(form, -1).astype(BF16)

    def conv2(i, frames):
        used = len(frames) * span
        m = [dot(w2_ref[k, :, 0:3 * channels], s_ref[i % 2, k, :, 0:used]) for k in range(4)]
        for parity, second in enumerate(((m[0] - m[1]) + m[2], (m[3] - m[1]) - m[2])):
            x = jnp.concatenate([second.astype(BF16), silu(second).astype(BF16)], axis=0)
            z = dot(wz_ref[...], x)
            for j, f in enumerate(frames):
                for p in range(pairs):
                    at = (j * pairs + p) * width
                    store(f, 2 * p + parity, z[:, at:at + width])

    conv1(0, batches[0])
    for i, frames in enumerate(batches):
        if i + 1 < len(batches):
            conv1(i + 1, batches[i + 1])
        conv2(i, frames)


def z_parts(z_ref, f, latent):
    return [z_ref[f, k * latent:(k + 1) * latent, :] for k in range(3)]


def step0_kernel(
    dims, frames, levels, tiles, keep_ref, noise_ref, prev_ref, own_ref, next_ref,
    w1_ref, w2_ref, wz_ref, upd_ref, fwd_ref, bwd_ref, s_ref, z_ref,
):
    latent, local_rows, width, channels = dims
    rows = local_rows + 4
    position = lax.rem(lax.axis_index("level") + levels - 1, levels)
    tile = lax.axis_index("tile")

    def latents(f):
        lo, hi = f * latent, (f + 1) * latent
        return jnp.concatenate(
            [
                prev_ref[lo:hi, (local_rows - 4) * width:], own_ref[lo:hi, :],
                next_ref[lo:hi, 0:4 * width],
            ],
            axis=1,
        ).astype(F32)

    def store(f, row, z):
        z_ref[f, :, row * width:(row + 1) * width] = z

    convolve(
        [(f,) for f in range(frames)], latents, dims, rows, tile, tiles,
        w1_ref, w2_ref, wz_ref, s_ref, store,
    )
    skip = 2 * width
    for f in range(frames):
        z = z_parts(z_ref, f, latent)[0]
        if f > 0:
            z = z + z_parts(z_ref, f - 1, latent)[1]
        if f + 1 < frames:
            z = z + z_parts(z_ref, f + 1, latent)[2]
        lo, hi = f * latent, (f + 1) * latent
        q = latents(f)[:, skip:skip + rows * width]
        upd = keep_ref[0, position, f] * q - noise_ref[0, position, f] * z
        upd_ref[lo:hi, :] = upd
        if f == 0:
            bwd_ref[0:latent, :] = z_parts(z_ref, 0, latent)[2]
            bwd_ref[latent:, :] = upd
        if f == frames - 1:
            fwd_ref[0:latent, :] = z_parts(z_ref, f, latent)[1]
            fwd_ref[latent:, :] = upd


def window(f, dims, frames, prev_ref, own_ref, next_ref):
    latent, local_rows, width, _ = dims
    lo, hi = (frames + f) * latent, (frames + f + 1) * latent
    return jnp.concatenate(
        [
            prev_ref[lo:hi, (local_rows - 2) * width:], own_ref[lo:hi, :],
            next_ref[lo:hi, 0:2 * width],
        ],
        axis=1,
    ).astype(F32)


def inside(v, dims, tile, tiles):
    local_rows, width = dims[1], dims[2]
    row = lax.broadcasted_iota(jnp.int32, v.shape, 1) // width
    low = jnp.where(tile == 0, 2, 0)
    high = jnp.where(tile == tiles - 1, 2 + local_rows, local_rows + 4)
    return jnp.where((row < low) | (row >= high), 0.0, v).astype(BF16).astype(F32)


def inner_kernel(
    dims, frames, levels, tiles, prev_ref, own_ref, next_ref, upd_ref,
    w1_ref, w2_ref, wz_ref, lat_ref, zin_ref, s_ref,
):
    latent, local_rows, width, channels = dims
    level, tile = lax.axis_index("level"), lax.axis_index("tile")

    def latents(f):
        fresh = window(f, dims, frames, prev_ref, own_ref, next_ref)
        v = jnp.where(level == 0, fresh, upd_ref[f * latent:(f + 1) * latent, :])
        v = inside(v, dims, tile, tiles)
        lat_ref[f - 1] = v[:, 2 * width:(2 + local_rows) * width]
        return v

    def store(f, row, z):
        zin_ref[f - 1, :, row * width:(row + 1) * width] = z

    inner = list(range(1, frames - 1))
    batches = [tuple(inner[k:k + 2]) for k in range(0, len(inner), 2)]
    convolve(
        batches, latents, dims, local_rows, tile, tiles, w1_ref, w2_ref, wz_ref, s_ref, store
    )


def outer_kernel(
    dims, frames, levels, tiles, keep_ref, noise_ref, prev_ref, own_ref, next_ref, upd_ref,
    fwd_ref, bwd_ref, fwd_in_ref, bwd_in_ref, lat_ref, zin_ref, w1_ref, w2_ref, wz_ref,
    out_ref, s_ref, z_ref, edge_ref,
):
    latent, local_rows, width, channels = dims
    level, tile = lax.axis_index("level"), lax.axis_index("tile")
    before = lax.rem(level + levels - 1, levels)
    last = frames - 1
    slots = {-1: 0, 0: 1, last: 2, frames: 3}

    def latents(f):
        fresh = window(min(max(f, 0), last) if f >= 0 else last,
                       dims, frames, prev_ref, own_ref, next_ref)
        if f == -1:
            earlier = lax.rem(level + levels - 2, levels)
            v = fwd_in_ref[latent:, :] - noise_ref[0, earlier, last] * bwd_ref[0:latent, :]
            v = jnp.where(level == 1, fresh, v)
            v = jnp.where(level == 0, 0.0, v)
        elif f == 0:
            rate = jnp.where(level == 1, 0.0, noise_ref[0, before, 0])
            v = upd_ref[0:latent, :] - rate * fwd_in_ref[0:latent, :]
            v = jnp.where(level == 0, fresh, v)
        elif f == last:
            v = upd_ref[last * latent:, :] - noise_ref[0, before, last] * bwd_in_ref[0:latent, :]
            v = jnp.where(level == 0, fresh, v)
        else:
            rate = jnp.where(level == 0, 0.0, noise_ref[0, level, 0])
            v = bwd_in_ref[latent:, :] - rate * fwd_ref[0:latent, :]
            v = jnp.where(level == levels - 1, 0.0, v)
        v = inside(v, dims, tile, tiles)
        edge_ref[slots[f]] = v[:, 2 * width:(2 + local_rows) * width]
        return v

    def store(f, row, z):
        z_ref[slots[f], :, row * width:(row + 1) * width] = z

    convolve(
        [(-1, 0), (last, frames)], latents, dims, local_rows, tile, tiles,
        w1_ref, w2_ref, wz_ref, s_ref, store,
    )

    def parts(f):
        if f in slots:
            return z_parts(z_ref, slots[f], latent)
        return z_parts(zin_ref, f - 1, latent)

    for f in range(frames):
        z = parts(f)[0] + parts(f - 1)[1] + parts(f + 1)[2]
        q = edge_ref[slots[f]] if f in slots else lat_ref[f - 1]
        out = keep_ref[1, level, f] * q - noise_ref[1, level, f] * z
        out_ref[f * latent:(f + 1) * latent, :] = out.astype(BF16)


def per_device(
    queue_init, noise_frames, conv_first, conv_second, time_weight, out_proj, keep_coef, noise_coef
):
    steps = noise_frames.shape[0]
    _, frames, latent, rows, width = queue_init.shape
    assert steps == 2 and rows >= 4 and rows % 2 == 0
    channels = conv_second.shape[2]
    levels, tiles = lax.axis_size("level"), lax.axis_size("tile")
    level = lax.axis_index("level")
    flat = frames * latent
    n_out, n_wide = rows * width, (rows + 4) * width
    dims = (latent, rows, width, channels)
    slot = slot_of(latent)

    smem = pl.BlockSpec(memory_space=pltpu.SMEM)
    vmem = pl.BlockSpec(memory_space=pltpu.VMEM)

    def shape(*dims_and_type):
        return jax.ShapeDtypeStruct(dims_and_type[:-1], dims_and_type[-1])

    def call(body, operands, scalars, outs, scratch, row_frames, grant):
        flops = 2 * row_frames * width * channels * 8 * channels
        return pl.pallas_call(
            body,
            out_shape=tuple(outs),
            in_specs=[smem] * scalars + [vmem] * (len(operands) - scalars),
            out_specs=(vmem,) * len(outs),
            scratch_shapes=scratch,
            compiler_params=pltpu.CompilerParams(vmem_limit_bytes=grant * MIB),
            cost_estimate=pl.CostEstimate(
                flops=flops, bytes_accessed=channels * channels * 24, transcendentals=0
            ),
        )(*operands)

    def permute(x, dl, dt):
        pairs = [
            (l * tiles + t, ((l + dl) % levels) * tiles + t + dt)
            for l in range(levels) for t in range(tiles) if 0 <= t + dt < tiles
        ]
        return lax.ppermute(x, ("level", "tile"), pairs)

    queue = queue_init[0].reshape(flat, n_out)
    noise = noise_frames.reshape(steps, flat, n_out)
    pack = jnp.concatenate([jnp.where(level == levels - 1, noise[0], queue), noise[1]], axis=0)
    own = permute(pack, 2, 0)
    prev = permute(pack, 2, 1)
    nxt = permute(pack, 2, -1)

    w1, w2, wz = call(
        prep_kernel,
        (
            conv_first.reshape(9, channels, latent), conv_second.reshape(9, channels, channels),
            time_weight, out_proj,
        ),
        0,
        [
            shape(channels, lanes(3 * slot), BF16), shape(4, channels, lanes(3 * channels), BF16),
            shape(4 * latent, 2 * channels, BF16),
        ],
        [], 4, 16,
    )
    weights = (w1, w2, wz)
    coefs = (keep_coef, noise_coef)
    around = (prev, own, nxt)

    def spare(pairs_of_rows):
        return pltpu.VMEM((2, 4, 3 * channels, pairs_of_rows * width), BF16)

    place = (dims, frames, levels, tiles)
    upd, fwd, bwd = call(
        functools.partial(step0_kernel, *place),
        coefs + around + weights, 2,
        [shape(flat, n_wide, F32)] + [shape(2 * latent, n_wide, F32)] * 2,
        [spare(rows // 2 + 2), pltpu.VMEM((frames, 4 * latent, n_wide), F32)],
        frames * (rows + 4), 32,
    )
    fwd_in = lax.ppermute(fwd, "level", [(l, l + 1) for l in range(1, levels - 1)])
    bwd_in = lax.ppermute(bwd, "level", [(l, (l - 1) % levels) for l in range(levels)])
    lat, zin = call(
        functools.partial(inner_kernel, *place),
        around + (upd,) + weights, 0,
        [shape(frames - 2, latent, n_out, F32), shape(frames - 2, 4 * latent, n_out, F32)],
        [spare(rows)], (frames - 2) * rows, 32,
    )
    (out,) = call(
        functools.partial(outer_kernel, *place),
        coefs + around + (upd, fwd, bwd, fwd_in, bwd_in, lat, zin) + weights, 2,
        [shape(flat, n_out, BF16)],
        [
            spare(rows), pltpu.VMEM((4, 4 * latent, n_out), F32),
            pltpu.VMEM((4, latent, n_out), F32),
        ],
        4 * rows, 32,
    )
    return out.reshape(1, frames, latent, rows, width)


def solution(mesh):
    return jax.shard_map(
        per_device,
        mesh=mesh,
        in_specs=(
            P("level", None, None, "tile", None),
            P(None, None, None, "tile", None),
            P(),
            P(),
            P(),
            P(),
            P(),
            P(),
        ),
        out_specs=P("level", None, None, "tile", None),
        check_vma=False,
    )
```

```python
import functools

import jax
import jax.numpy as jnp
from jax import lax
from jax.experimental import pallas as pl
from jax.experimental.pallas import tpu as pltpu
from jax.sharding import PartitionSpec as P

BF16 = jnp.bfloat16
F32 = jnp.float32
MIB = 1024 * 1024


def dot(a, b):
    return jnp.dot(a, b, preferred_element_type=F32)


def slot_of(latent):
    return -(-3 * latent // 16) * 16


def lanes(n):
    return -(-n // 128) * 128


def prep_kernel(
    first_hbm, second_hbm, time_hbm, proj_hbm, w1_ref, w2_ref, wz_ref,
    first_ref, second_ref, time_ref, proj_ref, second_sem, sems,
):
    taps, latent, channels = first_hbm.shape
    slot = slot_of(latent)
    loads = [
        pltpu.make_async_copy(src, dst, sems.at[k])
        for k, (src, dst) in enumerate(
            ((first_hbm, first_ref), (proj_hbm, proj_ref), (time_hbm, time_ref))
        )
    ]
    slabs = [
        pltpu.make_async_copy(second_hbm.at[k], second_ref.at[k], second_sem.at[k])
        for k in range(taps)
    ]
    for b in range(3):
        for a in range(3):
            slabs[3 * a + b].start()
    for load in loads:
        load.start()
    spare = w2_ref.shape[2] - 3 * channels
    if spare:
        w2_ref[:, :, 3 * channels:] = jnp.zeros((4, channels, spare), BF16)
    for b in range(3):
        for a in range(3):
            slabs[3 * a + b].wait()
        g = [0.5 * second_ref[3 * a + b].astype(F32) for a in range(3)]
        outer = 0.5 * (g[0] + g[2])
        middle = 0.5 * g[1]
        forms = [g[0], -outer - middle, outer - middle, -g[2]]
        for k in range(4):
            w2_ref[k, :, b * channels:(b + 1) * channels] = forms[k].astype(BF16)
    for load in loads:
        load.wait()
    pad = jnp.zeros((slot - 3 * latent, channels), F32)
    pieces = []
    for a in range(3):
        pieces += [first_ref[3 * a + b].astype(F32) for b in range(3)]
        if slot > 3 * latent:
            pieces.append(pad)
    w1 = 0.5 * jnp.concatenate(pieces, axis=0)
    w1 = jnp.pad(w1, ((0, w1_ref.shape[1] - 3 * slot), (0, lanes(channels) - channels)))
    w1_ref[...] = w1.T[0:channels].astype(BF16)
    proj = proj_ref[...]
    zero = jnp.zeros((latent, channels), F32)
    pt = [dot(proj, time_ref[k]) for k in range(3)]
    left = jnp.concatenate([2.0 * proj.astype(F32), zero, zero, zero], axis=0)
    right = jnp.concatenate([pt[1], pt[0], pt[2], zero], axis=0)
    wz_ref[:, 0:channels] = left.astype(BF16)
    wz_ref[:, channels:] = right.astype(BF16)


def gate(half):
    return half * jnp.tanh(half) + half


def convolve(batches, latents, dims, rows, tile, tiles, w1_ref, w2_ref, wz_ref, s_ref, store):
    latent, local_rows, width, channels = dims
    slot = slot_of(latent)
    pairs = rows // 2
    extra = (rows - local_rows) // 2
    span = pairs * width
    column = lax.broadcasted_iota(jnp.int32, (1, width), 1)
    not_first = jnp.where(column == 0, 0.0, 1.0)
    not_last = jnp.where(column == width - 1, 0.0, 1.0)
    top = jnp.where(tile == 0, 0.0, 1.0)
    bottom = jnp.where(tile == tiles - 1, 0.0, 1.0)

    def from_left(v):
        return pltpu.roll(v, 1, 1) * not_first.astype(v.dtype)

    def from_right(v):
        return pltpu.roll(v, width - 1, 1) * not_last.astype(v.dtype)

    def conv1(i, frames):
        for j, f in enumerate(frames):
            a = latents(f)
            b = []
            for r in range(rows + 4):
                v = a[:, r * width:(r + 1) * width]
                parts = [from_left(v), v, from_right(v)]
                if slot > 3 * latent:
                    parts.append(jnp.zeros((slot - 3 * latent, width), F32))
                b.append(jnp.concatenate(parts, axis=0))
            x = []
            for r in range(rows + 2):
                v = jnp.concatenate(b[r:r + 3], axis=0)
                if r <= extra:
                    v = v * top
                if r > extra + local_rows:
                    v = v * bottom
                x.append(v.astype(BF16))
            v = gate(dot(w1_ref[:, 0:3 * slot], jnp.concatenate(x, axis=1))).astype(BF16)
            d = [v[:, r * width:(r + 1) * width] for r in range(rows + 2)]
            for p in range(pairs):
                e = d[2 * p:2 * p + 4]
                at = slice(j * span + p * width, j * span + (p + 1) * width)
                for k, form in enumerate((e[0] - e[2], e[1] + e[2], e[2] - e[1], e[1] - e[3])):
                    s_ref[i % 2, k, 0:channels, at] = from_left(form)
                    s_ref[i % 2, k, channels:2 * channels, at] = form
                    s_ref[i % 2, k, 2 * channels:, at] = from_right(form)

    def conv2(i, frames):
        used = len(frames) * span
        m = [dot(w2_ref[k, :, 0:3 * channels], s_ref[i % 2, k, :, 0:used]) for k in range(4)]
        for parity, half in enumerate(((m[0] - m[1]) + m[2], (m[3] - m[1]) - m[2])):
            x = jnp.concatenate([half.astype(BF16), gate(half).astype(BF16)], axis=0)
            z = dot(wz_ref[...], x)
            for j, f in enumerate(frames):
                for p in range(pairs):
                    at = (j * pairs + p) * width
                    store(f, 2 * p + parity, z[:, at:at + width])

    conv1(0, batches[0])
    for i, frames in enumerate(batches):
        if i + 1 < len(batches):
            conv1(i + 1, batches[i + 1])
        conv2(i, frames)


def coef(ref, step, position, f):
    return ref[step, pl.ds(position, 1), f:f + 1]


def z_parts(z_ref, f, latent):
    return [z_ref[f, k * latent:(k + 1) * latent, :] for k in range(3)]


def step0_kernel(
    dims, frames, levels, tiles, keep_ref, noise_ref, prev_ref, own_ref, next_ref,
    w1_ref, w2_ref, wz_ref, upd_ref, fwd_ref, bwd_ref, s_ref, z_ref,
):
    latent, local_rows, width, channels = dims
    rows = local_rows + 4
    position = lax.rem(lax.axis_index("level") + levels - 1, levels)
    tile = lax.axis_index("tile")

    def latents(f):
        lo, hi = f * latent, (f + 1) * latent
        return jnp.concatenate(
            [
                prev_ref[lo:hi, (local_rows - 4) * width:], own_ref[lo:hi, :],
                next_ref[lo:hi, 0:4 * width],
            ],
            axis=1,
        ).astype(F32)

    def store(f, row, z):
        z_ref[f, :, row * width:(row + 1) * width] = z

    convolve(
        [(f,) for f in range(frames)], latents, dims, rows, tile, tiles,
        w1_ref, w2_ref, wz_ref, s_ref, store,
    )
    skip = 2 * width
    for f in range(frames):
        z = z_parts(z_ref, f, latent)[0]
        if f > 0:
            z = z + z_parts(z_ref, f - 1, latent)[1]
        if f + 1 < frames:
            z = z + z_parts(z_ref, f + 1, latent)[2]
        lo, hi = f * latent, (f + 1) * latent
        q = latents(f)[:, skip:skip + rows * width]
        upd = coef(keep_ref, 0, position, f) * q - coef(noise_ref, 0, position, f) * z
        upd_ref[lo:hi, :] = upd
        if f == 0:
            bwd_ref[0:latent, :] = z_parts(z_ref, 0, latent)[2]
            bwd_ref[latent:, :] = upd
        if f == frames - 1:
            fwd_ref[0:latent, :] = z_parts(z_ref, f, latent)[1]
            fwd_ref[latent:, :] = upd


def window(f, dims, frames, prev_ref, own_ref, next_ref):
    latent, local_rows, width, _ = dims
    lo, hi = (frames + f) * latent, (frames + f + 1) * latent
    return jnp.concatenate(
        [
            prev_ref[lo:hi, (local_rows - 2) * width:], own_ref[lo:hi, :],
            next_ref[lo:hi, 0:2 * width],
        ],
        axis=1,
    ).astype(F32)


def inside(v, dims, tile, tiles):
    local_rows, width = dims[1], dims[2]
    row = lax.broadcasted_iota(jnp.int32, v.shape, 1) // width
    low = jnp.where(tile == 0, 2, 0)
    high = jnp.where(tile == tiles - 1, 2 + local_rows, local_rows + 4)
    return jnp.where((row < low) | (row >= high), 0.0, v).astype(BF16).astype(F32)


def inner_kernel(
    dims, frames, levels, tiles, prev_ref, own_ref, next_ref, upd_ref,
    w1_ref, w2_ref, wz_ref, lat_ref, zin_ref, s_ref,
):
    latent, local_rows, width, channels = dims
    level, tile = lax.axis_index("level"), lax.axis_index("tile")

    def latents(f):
        fresh = window(f, dims, frames, prev_ref, own_ref, next_ref)
        v = jnp.where(level == 0, fresh, upd_ref[f * latent:(f + 1) * latent, :])
        v = inside(v, dims, tile, tiles)
        lat_ref[f - 1] = v[:, 2 * width:(2 + local_rows) * width]
        return v

    def store(f, row, z):
        zin_ref[f - 1, :, row * width:(row + 1) * width] = z

    inner = list(range(1, frames - 1))
    batches = [tuple(inner[k:k + 2]) for k in range(0, len(inner), 2)]
    convolve(
        batches, latents, dims, local_rows, tile, tiles, w1_ref, w2_ref, wz_ref, s_ref, store
    )


def outer_kernel(
    dims, frames, levels, tiles, keep_ref, noise_ref, prev_ref, own_ref, next_ref, upd_ref,
    fwd_ref, bwd_ref, fwd_in_ref, bwd_in_ref, lat_ref, zin_ref, w1_ref, w2_ref, wz_ref,
    out_ref, s_ref, z_ref, edge_ref,
):
    latent, local_rows, width, channels = dims
    level, tile = lax.axis_index("level"), lax.axis_index("tile")
    before = lax.rem(level + levels - 1, levels)
    last = frames - 1
    slots = {-1: 0, 0: 1, last: 2, frames: 3}

    def latents(f):
        fresh = window(min(max(f, 0), last) if f >= 0 else last,
                       dims, frames, prev_ref, own_ref, next_ref)
        if f == -1:
            earlier = lax.rem(level + levels - 2, levels)
            v = fwd_in_ref[latent:, :] - coef(noise_ref, 0, earlier, last) * bwd_ref[0:latent, :]
            v = jnp.where(level == 1, fresh, v)
            v = jnp.where(level == 0, 0.0, v)
        elif f == 0:
            rate = jnp.where(level == 1, 0.0, coef(noise_ref, 0, before, 0))
            v = upd_ref[0:latent, :] - rate * fwd_in_ref[0:latent, :]
            v = jnp.where(level == 0, fresh, v)
        elif f == last:
            v = upd_ref[last * latent:, :] - coef(noise_ref, 0, before, last) * bwd_in_ref[0:latent, :]
            v = jnp.where(level == 0, fresh, v)
        else:
            rate = jnp.where(level == 0, 0.0, coef(noise_ref, 0, level, 0))
            v = bwd_in_ref[latent:, :] - rate * fwd_ref[0:latent, :]
            v = jnp.where(level == levels - 1, 0.0, v)
        v = inside(v, dims, tile, tiles)
        edge_ref[slots[f]] = v[:, 2 * width:(2 + local_rows) * width]
        return v

    def store(f, row, z):
        z_ref[slots[f], :, row * width:(row + 1) * width] = z

    convolve(
        [(-1, 0), (last, frames)], latents, dims, local_rows, tile, tiles,
        w1_ref, w2_ref, wz_ref, s_ref, store,
    )

    def parts(f):
        if f in slots:
            return z_parts(z_ref, slots[f], latent)
        return z_parts(zin_ref, f - 1, latent)

    for f in range(frames):
        z = parts(f)[0] + parts(f - 1)[1] + parts(f + 1)[2]
        q = edge_ref[slots[f]] if f in slots else lat_ref[f - 1]
        out = coef(keep_ref, 1, level, f) * q - coef(noise_ref, 1, level, f) * z
        cut = [out[:, None, r * width:(r + 1) * width] for r in range(local_rows)]
        out_ref[f * latent:(f + 1) * latent] = jnp.concatenate(cut, axis=1).astype(BF16)


def per_device(
    queue_init, noise_frames, conv_first, conv_second, time_weight, out_proj, keep_coef, noise_coef
):
    steps = noise_frames.shape[0]
    _, frames, latent, rows, width = queue_init.shape
    assert steps == 2 and rows >= 4 and rows % 2 == 0
    channels = conv_second.shape[2]
    levels, tiles = lax.axis_size("level"), lax.axis_size("tile")
    level = lax.axis_index("level")
    flat = frames * latent
    n_out, n_wide = rows * width, (rows + 4) * width
    dims = (latent, rows, width, channels)
    slot = slot_of(latent)

    vmem = pl.BlockSpec(memory_space=pltpu.VMEM)

    def shape(*dims_and_type):
        return jax.ShapeDtypeStruct(dims_and_type[:-1], dims_and_type[-1])

    def call(body, operands, outs, scratch, row_frames, grant, space=vmem):
        flops = 2 * row_frames * width * channels * 8 * channels
        return pl.pallas_call(
            body,
            out_shape=tuple(outs),
            in_specs=[space] * len(operands),
            out_specs=(vmem,) * len(outs),
            scratch_shapes=scratch,
            compiler_params=pltpu.CompilerParams(vmem_limit_bytes=grant * MIB),
            cost_estimate=pl.CostEstimate(
                flops=flops, bytes_accessed=channels * channels * 24, transcendentals=0
            ),
        )(*operands)

    def in_hbm(x):
        return pltpu.with_memory_space_constraint(x, pltpu.HBM)

    def permute(x, dl, dt):
        pairs = [
            (l * tiles + t, ((l + dl) % levels) * tiles + t + dt)
            for l in range(levels) for t in range(tiles) if 0 <= t + dt < tiles
        ]
        return lax.ppermute(x, ("level", "tile"), pairs)

    queue = queue_init[0].reshape(flat, n_out)
    noise = noise_frames.reshape(steps, flat, n_out)
    pack = jnp.concatenate([jnp.where(level == levels - 1, noise[0], queue), noise[1]], axis=0)
    own = permute(pack, 2, 0)
    prev = permute(pack, 2, 1)
    nxt = permute(pack, 2, -1)

    second = conv_second.reshape(9, channels, channels)
    first = jnp.transpose(conv_first, (0, 1, 3, 2)).reshape(9, latent, channels)
    w1, w2, wz = call(
        prep_kernel,
        tuple(in_hbm(x) for x in (first, second, time_weight, out_proj)),
        [
            shape(channels, lanes(3 * slot), BF16), shape(4, channels, lanes(3 * channels), BF16),
            shape(4 * latent, 2 * channels, BF16),
        ],
        [pltpu.VMEM(x.shape, BF16) for x in (first, second, time_weight, out_proj)]
        + [pltpu.SemaphoreType.DMA((9,)), pltpu.SemaphoreType.DMA((3,))],
        4, 16, pl.BlockSpec(memory_space=pltpu.HBM),
    )
    weights = (w1, w2, wz)
    coefs = (keep_coef, noise_coef)
    around = (prev, own, nxt)

    def spare(pairs_of_rows):
        return pltpu.VMEM((2, 4, 3 * channels, pairs_of_rows * width), BF16)

    place = (dims, frames, levels, tiles)
    upd, fwd, bwd = call(
        functools.partial(step0_kernel, *place),
        coefs + around + weights,
        [shape(flat, n_wide, F32)] + [shape(2 * latent, n_wide, F32)] * 2,
        [spare(rows // 2 + 2), pltpu.VMEM((frames, 4 * latent, n_wide), F32)],
        frames * (rows + 4), 32,
    )
    fwd_in = lax.ppermute(fwd, "level", [(l, l + 1) for l in range(1, levels - 1)])
    bwd_in = lax.ppermute(bwd, "level", [(l, (l - 1) % levels) for l in range(levels)])
    lat, zin = call(
        functools.partial(inner_kernel, *place),
        around + (upd,) + weights,
        [shape(frames - 2, latent, n_out, F32), shape(frames - 2, 4 * latent, n_out, F32)],
        [spare(rows)], (frames - 2) * rows, 32,
    )
    (out,) = call(
        functools.partial(outer_kernel, *place),
        coefs + around + (upd, fwd, bwd, fwd_in, bwd_in, lat, zin) + weights,
        [shape(flat, rows, width, BF16)],
        [
            spare(rows), pltpu.VMEM((4, 4 * latent, n_out), F32),
            pltpu.VMEM((4, latent, n_out), F32),
        ],
        4 * rows, 32,
    )
    return out.reshape(1, frames, latent, rows, width)


def solution(mesh):
    return jax.shard_map(
        per_device,
        mesh=mesh,
        in_specs=(
            P("level", None, None, "tile", None),
            P(None, None, None, "tile", None),
            P(),
            P(),
            P(),
            P(),
            P(),
            P(),
        ),
        out_specs=P("level", None, None, "tile", None),
        check_vma=False,
    )
```

```python
import functools

import jax
import jax.numpy as jnp
from jax import lax
from jax.experimental import pallas as pl
from jax.experimental.pallas import tpu as pltpu
from jax.sharding import PartitionSpec as P

BF16 = jnp.bfloat16
F32 = jnp.float32
MIB = 1024 * 1024


def dot(a, b):
    return jnp.dot(a, b, preferred_element_type=F32)


def slot_of(latent):
    return -(-3 * latent // 16) * 16


def lanes(n):
    return -(-n // 128) * 128


def prep_kernel(
    first_hbm, second_hbm, time_hbm, proj_hbm, w1_ref, w2_ref, wz_ref,
    first_ref, second_ref, time_ref, proj_ref, second_sem, sems,
):
    taps, latent, channels = first_hbm.shape
    slot = slot_of(latent)
    loads = [
        pltpu.make_async_copy(src, dst, sems.at[k])
        for k, (src, dst) in enumerate(
            ((first_hbm, first_ref), (proj_hbm, proj_ref), (time_hbm, time_ref))
        )
    ]
    slabs = [
        pltpu.make_async_copy(second_hbm.at[k], second_ref.at[k], second_sem.at[k])
        for k in range(taps)
    ]
    for b in range(3):
        for a in range(3):
            slabs[3 * a + b].start()
    for load in loads:
        load.start()
    spare = w2_ref.shape[2] - 3 * channels
    if spare:
        w2_ref[:, :, 3 * channels:] = jnp.zeros((4, channels, spare), BF16)
    for b in range(3):
        for a in range(3):
            slabs[3 * a + b].wait()
        g = [0.5 * second_ref[3 * a + b].astype(F32) for a in range(3)]
        outer = 0.5 * (g[0] + g[2])
        middle = 0.5 * g[1]
        forms = [g[0], -outer - middle, outer - middle, -g[2]]
        for k in range(4):
            w2_ref[k, :, b * channels:(b + 1) * channels] = forms[k].astype(BF16)
    for load in loads:
        load.wait()
    pad = jnp.zeros((slot - 3 * latent, channels), F32)
    pieces = []
    for a in range(3):
        pieces += [first_ref[3 * a + b].astype(F32) for b in range(3)]
        if slot > 3 * latent:
            pieces.append(pad)
    w1 = 0.5 * jnp.concatenate(pieces, axis=0)
    w1 = jnp.pad(w1, ((0, w1_ref.shape[1] - 3 * slot), (0, lanes(channels) - channels)))
    w1_ref[...] = w1.T[0:channels].astype(BF16)
    proj = proj_ref[...]
    zero = jnp.zeros((latent, channels), F32)
    pt = [dot(proj, time_ref[k]) for k in range(3)]
    left = jnp.concatenate([2.0 * proj.astype(F32), zero, zero, zero], axis=0)
    right = jnp.concatenate([pt[1], pt[0], pt[2], zero], axis=0)
    wz_ref[:, 0:channels] = left.astype(BF16)
    wz_ref[:, channels:] = right.astype(BF16)


def gate(half):
    return half * jnp.tanh(half) + half


def convolve(batches, latents, dims, rows, tile, tiles, w1_ref, w2_ref, wz_ref, s_ref, store):
    latent, local_rows, width, channels = dims
    slot = slot_of(latent)
    pairs = rows // 2
    extra = (rows - local_rows) // 2
    span = pairs * width
    column = lax.broadcasted_iota(jnp.int32, (1, width), 1)
    not_first = jnp.where(column == 0, 0.0, 1.0)
    not_last = jnp.where(column == width - 1, 0.0, 1.0)
    top = jnp.where(tile == 0, 0.0, 1.0)
    bottom = jnp.where(tile == tiles - 1, 0.0, 1.0)

    def from_left(v):
        return pltpu.roll(v, 1, 1) * not_first.astype(v.dtype)

    def from_right(v):
        return pltpu.roll(v, width - 1, 1) * not_last.astype(v.dtype)

    def conv1(i, frames):
        for j, f in enumerate(frames):
            a = latents(f)
            b = []
            for r in range(rows + 4):
                v = a[:, r * width:(r + 1) * width]
                parts = [from_left(v), v, from_right(v)]
                if slot > 3 * latent:
                    parts.append(jnp.zeros((slot - 3 * latent, width), F32))
                b.append(jnp.concatenate(parts, axis=0))
            x = []
            for r in range(rows + 2):
                v = jnp.concatenate(b[r:r + 3], axis=0)
                if r <= extra:
                    v = v * top
                if r > extra + local_rows:
                    v = v * bottom
                x.append(v.astype(BF16))
            v = gate(dot(w1_ref[:, 0:3 * slot], jnp.concatenate(x, axis=1))).astype(BF16)
            d = [v[:, r * width:(r + 1) * width] for r in range(rows + 2)]
            for p in range(pairs):
                e = d[2 * p:2 * p + 4]
                at = slice(j * span + p * width, j * span + (p + 1) * width)
                for k, form in enumerate((e[0] - e[2], e[1] + e[2], e[2] - e[1], e[1] - e[3])):
                    s_ref[i % 2, k, 0:channels, at] = from_left(form)
                    s_ref[i % 2, k, channels:2 * channels, at] = form
                    s_ref[i % 2, k, 2 * channels:, at] = from_right(form)

    def conv2(i, frames):
        used = len(frames) * span
        m = [dot(w2_ref[k, :, 0:3 * channels], s_ref[i % 2, k, :, 0:used]) for k in range(4)]
        for parity, half in enumerate(((m[0] - m[1]) + m[2], (m[3] - m[1]) - m[2])):
            x = jnp.concatenate([half.astype(BF16), gate(half).astype(BF16)], axis=0)
            z = dot(wz_ref[...], x)
            for j, f in enumerate(frames):
                for p in range(pairs):
                    at = (j * pairs + p) * width
                    store(f, 2 * p + parity, z[:, at:at + width])

    conv1(0, batches[0])
    for i, frames in enumerate(batches):
        if i + 1 < len(batches):
            conv1(i + 1, batches[i + 1])
        conv2(i, frames)


def neighbours(odd_ref, even_ref, tile, lo, hi):
    odd, even = odd_ref[lo:hi, :].astype(F32), even_ref[lo:hi, :].astype(F32)
    is_even = lax.rem(tile, 2) == 0
    return jnp.where(is_even, odd, even), jnp.where(is_even, even, odd)


def coef(ref, step, position, f):
    return ref[step, pl.ds(position, 1), f:f + 1]


def z_parts(z_ref, f, latent):
    return [z_ref[f, k * latent:(k + 1) * latent, :] for k in range(3)]


def step0_kernel(
    dims, frames, levels, tiles, keep_ref, noise_ref, odd_ref, own_ref, even_ref,
    w1_ref, w2_ref, wz_ref, full_ref, near_ref, far_ref, s_ref, z_ref,
):
    latent, local_rows, width, channels = dims
    rows = local_rows + 4
    level = lax.axis_index("level")
    position = lax.rem(level + 1, levels)
    even = lax.rem(level, 2) == 0
    flat = frames * latent
    tile = lax.axis_index("tile")

    def latents(f):
        lo, hi = f * latent, (f + 1) * latent
        prev, after = neighbours(odd_ref, even_ref, tile, lo, hi)
        own = own_ref[lo:hi, :].astype(F32)
        return jnp.concatenate(
            [prev[:, (local_rows - 4) * width:], own, after[:, 0:4 * width]], axis=1
        )

    def store(f, row, z):
        z_ref[f, :, row * width:(row + 1) * width] = z

    convolve(
        [(f,) for f in range(frames)], latents, dims, rows, tile, tiles,
        w1_ref, w2_ref, wz_ref, s_ref, store,
    )
    skip = 2 * width
    for f in range(frames):
        z = z_parts(z_ref, f, latent)[0]
        if f > 0:
            z = z + z_parts(z_ref, f - 1, latent)[1]
        if f + 1 < frames:
            z = z + z_parts(z_ref, f + 1, latent)[2]
        lo, hi = f * latent, (f + 1) * latent
        q = latents(f)[:, skip:skip + rows * width]
        upd = coef(keep_ref, 0, position, f) * q - coef(noise_ref, 0, position, f) * z
        full_ref[lo:hi, :] = upd
        if f == 0:
            first = jnp.concatenate([z_parts(z_ref, 0, latent)[2], upd], axis=0)
        if f == frames - 1:
            last = jnp.concatenate([z_parts(z_ref, f, latent)[1], upd], axis=0)
    full_ref[flat:flat + latent, :] = last[0:latent]
    full_ref[flat + latent:, :] = first[0:latent]
    near_ref[...] = jnp.where(even, first, last)
    far_ref[...] = jnp.where(even, last, first)


def window(f, dims, frames, tile, odd_ref, own_ref, even_ref):
    latent, local_rows, width, _ = dims
    lo, hi = (frames + f) * latent, (frames + f + 1) * latent
    prev, after = neighbours(odd_ref, even_ref, tile, lo, hi)
    own = own_ref[lo:hi, :].astype(F32)
    return jnp.concatenate(
        [prev[:, (local_rows - 2) * width:], own, after[:, 0:2 * width]], axis=1
    )


def inside(v, dims, tile, tiles):
    local_rows, width = dims[1], dims[2]
    row = lax.broadcasted_iota(jnp.int32, v.shape, 1) // width
    low = jnp.where(tile == 0, 2, 0)
    high = jnp.where(tile == tiles - 1, 2 + local_rows, local_rows + 4)
    return jnp.where((row < low) | (row >= high), 0.0, v).astype(BF16).astype(F32)


def inner_kernel(
    dims, frames, levels, tiles, odd_ref, own_ref, even_ref, upd_ref,
    w1_ref, w2_ref, wz_ref, lat_ref, zin_ref, s_ref,
):
    latent, local_rows, width, channels = dims
    level, tile = lax.axis_index("level"), lax.axis_index("tile")

    def latents(f):
        fresh = window(f, dims, frames, tile, odd_ref, own_ref, even_ref)
        v = jnp.where(level == 0, fresh, upd_ref[f * latent:(f + 1) * latent, :])
        v = inside(v, dims, tile, tiles)
        lat_ref[f - 1] = v[:, 2 * width:(2 + local_rows) * width]
        return v

    def store(f, row, z):
        zin_ref[f - 1, :, row * width:(row + 1) * width] = z

    inner = list(range(1, frames - 1))
    batches = [tuple(inner[k:k + 2]) for k in range(0, len(inner), 2)]
    convolve(
        batches, latents, dims, local_rows, tile, tiles, w1_ref, w2_ref, wz_ref, s_ref, store
    )


def outer_kernel(
    dims, frames, levels, tiles, keep_ref, noise_ref, odd_ref, own_ref, even_ref, upd_ref,
    near_ref, far_ref, lat_ref, zin_ref, w1_ref, w2_ref, wz_ref,
    out_ref, s_ref, z_ref, edge_ref,
):
    latent, local_rows, width, channels = dims
    level, tile = lax.axis_index("level"), lax.axis_index("tile")
    before = lax.rem(level + levels - 1, levels)
    last = frames - 1
    flat = frames * latent
    even = lax.rem(level, 2) == 0
    fwd, bwd = upd_ref[flat:flat + latent, :], upd_ref[flat + latent:, :]
    near, far = near_ref[...], far_ref[...]
    fwd_in, bwd_in = jnp.where(even, near, far), jnp.where(even, far, near)
    slots = {-1: 0, 0: 1, last: 2, frames: 3}

    def latents(f):
        source = last if f < 0 else min(f, last)
        fresh = window(source, dims, frames, tile, odd_ref, own_ref, even_ref)
        if f == -1:
            earlier = lax.rem(level + levels - 2, levels)
            v = fwd_in[latent:] - coef(noise_ref, 0, earlier, last) * bwd
            v = jnp.where(level == 1, fresh, v)
            v = jnp.where(level == 0, 0.0, v)
        elif f == 0:
            rate = jnp.where(level == 1, 0.0, coef(noise_ref, 0, before, 0))
            v = upd_ref[0:latent, :] - rate * fwd_in[0:latent]
            v = jnp.where(level == 0, fresh, v)
        elif f == last:
            v = upd_ref[last * latent:flat, :] - coef(noise_ref, 0, before, last) * bwd_in[0:latent]
            v = jnp.where(level == 0, fresh, v)
        else:
            rate = jnp.where(level == 0, 0.0, coef(noise_ref, 0, level, 0))
            v = bwd_in[latent:] - rate * fwd
            v = jnp.where(level == levels - 1, 0.0, v)
        v = inside(v, dims, tile, tiles)
        edge_ref[slots[f]] = v[:, 2 * width:(2 + local_rows) * width]
        return v

    def store(f, row, z):
        z_ref[slots[f], :, row * width:(row + 1) * width] = z

    convolve(
        [(-1, 0), (last, frames)], latents, dims, local_rows, tile, tiles,
        w1_ref, w2_ref, wz_ref, s_ref, store,
    )

    def parts(f):
        if f in slots:
            return z_parts(z_ref, slots[f], latent)
        return z_parts(zin_ref, f - 1, latent)

    for f in range(frames):
        z = parts(f)[0] + parts(f - 1)[1] + parts(f + 1)[2]
        q = edge_ref[slots[f]] if f in slots else lat_ref[f - 1]
        out = coef(keep_ref, 1, level, f) * q - coef(noise_ref, 1, level, f) * z
        cut = [out[:, None, r * width:(r + 1) * width] for r in range(local_rows)]
        out_ref[f * latent:(f + 1) * latent] = jnp.concatenate(cut, axis=1).astype(BF16)


def per_device(
    queue_init, noise_frames, conv_first, conv_second, time_weight, out_proj, keep_coef, noise_coef
):
    steps = noise_frames.shape[0]
    _, frames, latent, rows, width = queue_init.shape
    assert steps == 2 and rows >= 4 and rows % 2 == 0
    channels = conv_second.shape[2]
    levels, tiles = lax.axis_size("level"), lax.axis_size("tile")
    level = lax.axis_index("level")
    flat = frames * latent
    n_out, n_wide = rows * width, (rows + 4) * width
    dims = (latent, rows, width, channels)
    slot = slot_of(latent)

    vmem = pl.BlockSpec(memory_space=pltpu.VMEM)

    def shape(*dims_and_type):
        return jax.ShapeDtypeStruct(dims_and_type[:-1], dims_and_type[-1])

    def call(body, operands, outs, scratch, row_frames, grant, space=vmem):
        flops = 2 * row_frames * width * channels * 8 * channels
        return pl.pallas_call(
            body,
            out_shape=tuple(outs),
            in_specs=[space] * len(operands),
            out_specs=(vmem,) * len(outs),
            scratch_shapes=scratch,
            compiler_params=pltpu.CompilerParams(vmem_limit_bytes=grant * MIB),
            cost_estimate=pl.CostEstimate(
                flops=flops, bytes_accessed=channels * channels * 24, transcendentals=0
            ),
        )(*operands)

    def in_hbm(x):
        return pltpu.with_memory_space_constraint(x, pltpu.HBM)

    def swap(x, axis, size, partner):
        pairs = [(i, partner(i)) for i in range(size) if 0 <= partner(i) < size]
        return lax.ppermute(x, axis, pairs)

    queue = queue_init[0].reshape(flat, n_out)
    noise = noise_frames.reshape(steps, flat, n_out)
    pack = jnp.concatenate([jnp.where(level == levels - 1, noise[0], queue), noise[1]], axis=0)
    own = pack
    odd = swap(pack, "tile", tiles, lambda t: t - 1 if t % 2 == 0 else t + 1)
    even = swap(pack, "tile", tiles, lambda t: t + 1 if t % 2 == 0 else t - 1)

    second = conv_second.reshape(9, channels, channels)
    first = jnp.transpose(conv_first, (0, 1, 3, 2)).reshape(9, latent, channels)
    w1, w2, wz = call(
        prep_kernel,
        tuple(in_hbm(x) for x in (first, second, time_weight, out_proj)),
        [
            shape(channels, lanes(3 * slot), BF16), shape(4, channels, lanes(3 * channels), BF16),
            shape(4 * latent, 2 * channels, BF16),
        ],
        [pltpu.VMEM(x.shape, BF16) for x in (first, second, time_weight, out_proj)]
        + [pltpu.SemaphoreType.DMA((9,)), pltpu.SemaphoreType.DMA((3,))],
        4, 16, pl.BlockSpec(memory_space=pltpu.HBM),
    )
    weights = (w1, w2, wz)
    coefs = (keep_coef, noise_coef)
    around = (odd, own, even)

    def spare(pairs_of_rows):
        return pltpu.VMEM((2, 4, 3 * channels, pairs_of_rows * width), BF16)

    place = (dims, frames, levels, tiles)
    full, near, far = call(
        functools.partial(step0_kernel, *place),
        coefs + around + weights,
        [shape(flat + 2 * latent, n_wide, F32)] + [shape(2 * latent, n_wide, F32)] * 2,
        [spare(rows // 2 + 2), pltpu.VMEM((frames, 4 * latent, n_wide), F32)],
        frames * (rows + 4), 32,
    )
    upd = swap(full, "level", levels, lambda d: (d + 2) % levels)
    far = swap(far, "level", levels, lambda d: (d - 1 if d % 2 == 0 else d + 1) % levels)
    near = swap(near, "level", levels, lambda d: d + 1 if d % 2 == 0 else d - 1)
    lat, zin = call(
        functools.partial(inner_kernel, *place),
        around + (upd,) + weights,
        [shape(frames - 2, latent, n_out, F32), shape(frames - 2, 4 * latent, n_out, F32)],
        [spare(rows)], (frames - 2) * rows, 32,
    )
    (out,) = call(
        functools.partial(outer_kernel, *place),
        coefs + around + (upd, near, far, lat, zin) + weights,
        [shape(flat, rows, width, BF16)],
        [
            spare(rows), pltpu.VMEM((4, 4 * latent, n_out), F32),
            pltpu.VMEM((4, latent, n_out), F32),
        ],
        4 * rows, 32,
    )
    return out.reshape(1, frames, latent, rows, width)


def solution(mesh):
    return jax.shard_map(
        per_device,
        mesh=mesh,
        in_specs=(
            P("level", None, None, "tile", None),
            P(None, None, None, "tile", None),
            P(),
            P(),
            P(),
            P(),
            P(),
            P(),
        ),
        out_specs=P("level", None, None, "tile", None),
        check_vma=False,
    )
```

```python
import functools

import jax
import jax.numpy as jnp
from jax import lax
from jax.experimental import pallas as pl
from jax.experimental.pallas import tpu as pltpu
from jax.sharding import PartitionSpec as P

BF16 = jnp.bfloat16
F32 = jnp.float32
MIB = 1024 * 1024
AHEAD, SLOTS = 1, 2
TILE, FORMS = 4, 6


def dot(a, b):
    return jnp.dot(a, b, preferred_element_type=F32)


def slot_of(latent):
    return -(-3 * latent // 16) * 16


def lanes(n):
    return -(-n // 128) * 128


def prep_kernel(
    first_hbm, second_hbm, time_hbm, proj_hbm, keep_hbm, noise_hbm,
    w1_ref, w2_ref, wz_ref, keep_ref, noise_ref,
    first_ref, second_ref, time_ref, proj_ref, second_sem, sems,
):
    taps, latent, channels = first_hbm.shape
    slot = slot_of(latent)
    main = channels // 128 * 128
    loads = [
        pltpu.make_async_copy(src, dst, sems.at[k])
        for k, (src, dst) in enumerate(
            (
                (first_hbm, first_ref), (proj_hbm, proj_ref), (time_hbm, time_ref),
                (keep_hbm, keep_ref), (noise_hbm, noise_ref),
            )
        )
    ]
    slabs = [
        pltpu.make_async_copy(second_hbm.at[k], second_ref.at[k], second_sem.at[k])
        for k in range(taps)
    ]
    for b in range(3):
        for a in range(3):
            slabs[3 * a + b].start()
    for load in loads:
        load.start()
    full_blocks, tail = main // 128, channels - main
    blocks = w2_ref.shape[1]
    spare = blocks * 128 - 3 * channels
    if spare:
        w2_ref[:, blocks - 1, :, 128 - spare:] = jnp.zeros((FORMS, channels, spare), BF16)
    for b in range(3):
        for a in range(3):
            slabs[3 * a + b].wait()
        for lo in range(0, channels, 32):
            at = slice(lo, min(lo + 32, channels))
            g = [second_ref[3 * a + b, at].astype(F32) for a in range(3)]
            ends = g[0] + g[2]
            far_ends, middle = g[0] + 4.0 * g[2], 2.0 * g[1]
            forms = [
                0.125 * g[0], (1.0 / 12.0) * (ends + g[1]), (-1.0 / 24.0) * (ends - g[1]),
                (-1.0 / 48.0) * (far_ends + middle), (1.0 / 96.0) * (far_ends - middle),
                0.5 * g[2],
            ]
            for k, form in enumerate(forms):
                form = form.astype(BF16)
                for t in range(full_blocks):
                    w2_ref[k, b * full_blocks + t, at] = form[:, t * 128:(t + 1) * 128]
                start = 0
                while start < tail:
                    lane = b * tail + start
                    size = min(tail - start, 128 - lane % 128)
                    w2_ref[k, 3 * full_blocks + lane // 128, at, lane % 128:lane % 128 + size] = (
                        form[:, main + start:main + start + size]
                    )
                    start += size
    for load in loads:
        load.wait()
    pad = jnp.zeros((slot - 3 * latent, channels), F32)
    pieces = []
    for a in range(3):
        pieces += [first_ref[3 * a + b].astype(F32) for b in range(3)]
        if slot > 3 * latent:
            pieces.append(pad)
    w1 = 0.5 * jnp.concatenate(pieces, axis=0)
    w1 = jnp.pad(w1, ((0, w1_ref.shape[1] - 3 * slot), (0, lanes(channels) - channels)))
    w1_ref[...] = w1.T[0:channels].astype(BF16)
    proj = proj_ref[...]
    zero = jnp.zeros((latent, channels), F32)
    pt = [dot(proj, time_ref[k]) for k in range(3)]
    left = jnp.concatenate([2.0 * proj.astype(F32), zero, zero, zero], axis=0)
    right = jnp.concatenate([pt[1], pt[0], pt[2], zero], axis=0)
    wz_ref[:, 0:channels] = left.astype(BF16)
    wz_ref[:, channels:] = right.astype(BF16)


def row_forms(d):
    low = 4.0 * d[1]
    even1, odd1 = d[4] - 4.0 * d[2], d[3] - low
    even2, odd2 = d[4] - d[2], 2.0 * (d[3] - d[1])
    return (
        4.0 * d[0] + (even1 - d[2]), even1 + odd1, even1 - odd1, even2 + odd2, even2 - odd2,
        low + (d[5] - 5.0 * d[3]),
    )


def row_sums(product, put):
    n, h = product(1), 2.0 * product(2)
    even1, odd1 = n - h, n + h
    n, h = product(3), 2.0 * product(4)
    even2, odd2 = n - h, n + h
    put(1, -2.0 * odd2 - odd1)
    put(2, -4.0 * even2 - even1)
    put(0, (product(0) - even1) - even2)
    put(3, (product(5) - odd1) - 8.0 * odd2)


def gate(half):
    return half * jnp.tanh(half) + half


def convolve(batches, latents, dims, rows, tile, tiles, w1_ref, w2_ref, wz_ref, s_ref, store):
    latent, local_rows, width, channels = dims
    slot = slot_of(latent)
    parts_per = rows // TILE
    main = channels // 128 * 128
    extra = (rows - local_rows) // 2
    span = parts_per * width
    column = lax.broadcasted_iota(jnp.int32, (1, width), 1)
    not_first = jnp.where(column == 0, 0.0, 1.0)
    not_last = jnp.where(column == width - 1, 0.0, 1.0)
    top = jnp.where(tile == 0, 0.0, 1.0)
    bottom = jnp.where(tile == tiles - 1, 0.0, 1.0)

    def from_left(v):
        return pltpu.roll(v, 1, 1) * not_first.astype(v.dtype)

    def from_right(v):
        return pltpu.roll(v, width - 1, 1) * not_last.astype(v.dtype)

    def conv1(i, frames):
        for j, f in enumerate(frames):
            a = latents(f)
            b = []
            for r in range(rows + 4):
                v = a[:, r * width:(r + 1) * width]
                parts = [from_left(v), v, from_right(v)]
                if slot > 3 * latent:
                    parts.append(jnp.zeros((slot - 3 * latent, width), F32))
                b.append(jnp.concatenate(parts, axis=0))
            x = []
            for r in range(rows + 2):
                v = jnp.concatenate(b[r:r + 3], axis=0)
                if r <= extra:
                    v = v * top
                if r > extra + local_rows:
                    v = v * bottom
                x.append(v.astype(BF16))
            v = gate(dot(w1_ref[:, 0:3 * slot], jnp.concatenate(x, axis=1)))
            d = [v[:, r * width:(r + 1) * width] for r in range(rows + 2)]
            for p in range(parts_per):
                at = j * parts_per + p
                for k, form in enumerate(row_forms(d[TILE * p:TILE * p + FORMS])):
                    form = form.astype(BF16)
                    for c, v in enumerate((from_left(form), form, from_right(form))):
                        tail = 3 * main + c * (channels - main)
                        s_ref[i % SLOTS, k, at, c * main:(c + 1) * main, :] = v[0:main]
                        if main < channels:
                            s_ref[i % SLOTS, k, at, tail:tail + channels - main, :] = v[main:]

    def conv2(i, frames):
        def product(k):
            x = [s_ref[i % SLOTS, k, p] for p in range(len(frames) * parts_per)]
            w = jnp.concatenate([w2_ref[k, t] for t in range(w2_ref.shape[1])], axis=1)
            return dot(w[:, 0:3 * channels], jnp.concatenate(x, axis=1))

        ready = {}

        def put(r, half):
            ready[r] = jnp.concatenate([half.astype(BF16), gate(half).astype(BF16)], axis=0)

        row_sums(product, put)
        return ready

    def project(frames, ready):
        for r, x in ready.items():
            z = dot(wz_ref[...], x)
            for j, f in enumerate(frames):
                for p in range(parts_per):
                    at = (j * parts_per + p) * width
                    store(f, TILE * p + r, z[:, at:at + width])

    count = len(batches)
    for i in range(min(AHEAD, count)):
        conv1(i, batches[i])
    for i in range(count):
        if AHEAD == 1 and i + 1 < count:
            conv1(i + 1, batches[i + 1])
        ready = conv2(i, batches[i])
        if AHEAD == 2 and i + 2 < count:
            conv1(i + 2, batches[i + 2])
        project(batches[i], ready)


def neighbours(odd_ref, even_ref, tile, lo, hi):
    odd, even = odd_ref[lo:hi, :].astype(F32), even_ref[lo:hi, :].astype(F32)
    is_even = lax.rem(tile, 2) == 0
    return jnp.where(is_even, odd, even), jnp.where(is_even, even, odd)


def coef(ref, step, position, f):
    return ref[step, pl.ds(position, 1), f:f + 1]


def z_parts(z_ref, f, latent):
    return [z_ref[f, k * latent:(k + 1) * latent, :] for k in range(3)]


def step0_kernel(
    dims, frames, levels, tiles, keep_ref, noise_ref, odd_ref, own_ref, even_ref,
    w1_ref, w2_ref, wz_ref, full_ref, near_ref, far_ref, s_ref, z_ref,
):
    latent, local_rows, width, channels = dims
    rows = local_rows + 4
    level = lax.axis_index("level")
    position = lax.rem(level + 1, levels)
    even = lax.rem(level, 2) == 0
    flat = frames * latent
    tile = lax.axis_index("tile")

    def latents(f):
        lo, hi = f * latent, (f + 1) * latent
        prev, after = neighbours(odd_ref, even_ref, tile, lo, hi)
        own = own_ref[lo:hi, :].astype(F32)
        return jnp.concatenate(
            [prev[:, (local_rows - 4) * width:], own, after[:, 0:4 * width]], axis=1
        )

    def store(f, row, z):
        z_ref[f, :, row * width:(row + 1) * width] = z

    convolve(
        [(f,) for f in range(frames)], latents, dims, rows, tile, tiles,
        w1_ref, w2_ref, wz_ref, s_ref, store,
    )
    skip = 2 * width
    for f in range(frames):
        z = z_parts(z_ref, f, latent)[0]
        if f > 0:
            z = z + z_parts(z_ref, f - 1, latent)[1]
        if f + 1 < frames:
            z = z + z_parts(z_ref, f + 1, latent)[2]
        lo, hi = f * latent, (f + 1) * latent
        q = latents(f)[:, skip:skip + rows * width]
        upd = coef(keep_ref, 0, position, f) * q - coef(noise_ref, 0, position, f) * z
        full_ref[lo:hi, :] = upd
        if f == 0:
            first = jnp.concatenate([z_parts(z_ref, 0, latent)[2], upd], axis=0)
        if f == frames - 1:
            last = jnp.concatenate([z_parts(z_ref, f, latent)[1], upd], axis=0)
    full_ref[flat:flat + latent, :] = last[0:latent]
    full_ref[flat + latent:, :] = first[0:latent]
    near_ref[...] = jnp.where(even, first, last)
    far_ref[...] = jnp.where(even, last, first)


def window(f, dims, frames, tile, odd_ref, own_ref, even_ref):
    latent, local_rows, width, _ = dims
    lo, hi = (frames + f) * latent, (frames + f + 1) * latent
    prev, after = neighbours(odd_ref, even_ref, tile, lo, hi)
    own = own_ref[lo:hi, :].astype(F32)
    return jnp.concatenate(
        [prev[:, (local_rows - 2) * width:], own, after[:, 0:2 * width]], axis=1
    )


def inside(v, dims, tile, tiles):
    local_rows, width = dims[1], dims[2]
    row = lax.broadcasted_iota(jnp.int32, v.shape, 1) // width
    low = jnp.where(tile == 0, 2, 0)
    high = jnp.where(tile == tiles - 1, 2 + local_rows, local_rows + 4)
    return jnp.where((row < low) | (row >= high), 0.0, v).astype(BF16).astype(F32)


def inner_kernel(
    dims, frames, levels, tiles, odd_ref, own_ref, even_ref, upd_ref,
    w1_ref, w2_ref, wz_ref, lat_ref, zin_ref, s_ref,
):
    latent, local_rows, width, channels = dims
    level, tile = lax.axis_index("level"), lax.axis_index("tile")

    def latents(f):
        fresh = window(f, dims, frames, tile, odd_ref, own_ref, even_ref)
        v = jnp.where(level == 0, fresh, upd_ref[f * latent:(f + 1) * latent, :])
        v = inside(v, dims, tile, tiles)
        lat_ref[f - 1] = v[:, 2 * width:(2 + local_rows) * width]
        return v

    def store(f, row, z):
        zin_ref[f - 1, :, row * width:(row + 1) * width] = z

    inner = list(range(1, frames - 1))
    batches = [tuple(inner[k:k + 2]) for k in range(0, len(inner), 2)]
    convolve(
        batches, latents, dims, local_rows, tile, tiles, w1_ref, w2_ref, wz_ref, s_ref, store
    )


def outer_kernel(
    dims, frames, levels, tiles, keep_ref, noise_ref, odd_ref, own_ref, even_ref, upd_ref,
    near_ref, far_ref, lat_ref, zin_ref, w1_ref, w2_ref, wz_ref,
    out_ref, s_ref, z_ref, edge_ref,
):
    latent, local_rows, width, channels = dims
    level, tile = lax.axis_index("level"), lax.axis_index("tile")
    before = lax.rem(level + levels - 1, levels)
    last = frames - 1
    flat = frames * latent
    even = lax.rem(level, 2) == 0
    fwd, bwd = upd_ref[flat:flat + latent, :], upd_ref[flat + latent:, :]
    near, far = near_ref[...], far_ref[...]
    fwd_in, bwd_in = jnp.where(even, near, far), jnp.where(even, far, near)
    slots = {-1: 0, 0: 1, last: 2, frames: 3}

    def latents(f):
        source = last if f < 0 else min(f, last)
        fresh = window(source, dims, frames, tile, odd_ref, own_ref, even_ref)
        if f == -1:
            earlier = lax.rem(level + levels - 2, levels)
            v = fwd_in[latent:] - coef(noise_ref, 0, earlier, last) * bwd
            v = jnp.where(level == 1, fresh, v)
            v = jnp.where(level == 0, 0.0, v)
        elif f == 0:
            rate = jnp.where(level == 1, 0.0, coef(noise_ref, 0, before, 0))
            v = upd_ref[0:latent, :] - rate * fwd_in[0:latent]
            v = jnp.where(level == 0, fresh, v)
        elif f == last:
            v = upd_ref[last * latent:flat, :] - coef(noise_ref, 0, before, last) * bwd_in[0:latent]
            v = jnp.where(level == 0, fresh, v)
        else:
            rate = jnp.where(level == 0, 0.0, coef(noise_ref, 0, level, 0))
            v = bwd_in[latent:] - rate * fwd
            v = jnp.where(level == levels - 1, 0.0, v)
        v = inside(v, dims, tile, tiles)
        edge_ref[slots[f]] = v[:, 2 * width:(2 + local_rows) * width]
        return v

    def store(f, row, z):
        z_ref[slots[f], :, row * width:(row + 1) * width] = z

    convolve(
        [(-1, 0), (last, frames)], latents, dims, local_rows, tile, tiles,
        w1_ref, w2_ref, wz_ref, s_ref, store,
    )

    def parts(f):
        if f in slots:
            return z_parts(z_ref, slots[f], latent)
        return z_parts(zin_ref, f - 1, latent)

    for f in range(frames):
        z = parts(f)[0] + parts(f - 1)[1] + parts(f + 1)[2]
        q = edge_ref[slots[f]] if f in slots else lat_ref[f - 1]
        out = coef(keep_ref, 1, level, f) * q - coef(noise_ref, 1, level, f) * z
        cut = [out[:, None, r * width:(r + 1) * width] for r in range(local_rows)]
        out_ref[f * latent:(f + 1) * latent] = jnp.concatenate(cut, axis=1).astype(BF16)


def per_device(
    queue_init, noise_frames, conv_first, conv_second, time_weight, out_proj, keep_coef, noise_coef
):
    steps = noise_frames.shape[0]
    _, frames, latent, rows, width = queue_init.shape
    channels = conv_second.shape[2]
    levels, tiles = lax.axis_size("level"), lax.axis_size("tile")
    level = lax.axis_index("level")
    assert steps == 2 and rows % TILE == 0 and levels % 4 == 0
    flat = frames * latent
    n_out, n_wide = rows * width, (rows + 4) * width
    dims = (latent, rows, width, channels)
    slot = slot_of(latent)

    vmem = pl.BlockSpec(memory_space=pltpu.VMEM)

    def shape(*dims_and_type):
        return jax.ShapeDtypeStruct(dims_and_type[:-1], dims_and_type[-1])

    def call(body, operands, outs, scratch, row_frames, grant, space=vmem):
        flops = 2 * row_frames * width * channels * 8 * channels
        return pl.pallas_call(
            body,
            out_shape=tuple(outs),
            in_specs=[space] * len(operands),
            out_specs=(vmem,) * len(outs),
            scratch_shapes=scratch,
            compiler_params=pltpu.CompilerParams(vmem_limit_bytes=grant * MIB),
            cost_estimate=pl.CostEstimate(
                flops=flops, bytes_accessed=channels * channels * 24, transcendentals=0
            ),
        )(*operands)

    def in_hbm(x):
        return pltpu.with_memory_space_constraint(x, pltpu.HBM)

    def swap(x, axis, size, partner):
        pairs = [(i, partner(i)) for i in range(size) if 0 <= partner(i) < size]
        return lax.ppermute(x, axis, pairs)

    queue = queue_init[0].reshape(flat, n_out)
    noise = noise_frames.reshape(steps, flat, n_out)
    pack = jnp.concatenate([jnp.where(level == levels - 1, noise[0], queue), noise[1]], axis=0)
    own = pack
    odd = swap(pack, "tile", tiles, lambda t: t - 1 if t % 2 == 0 else t + 1)
    even = swap(pack, "tile", tiles, lambda t: t + 1 if t % 2 == 0 else t - 1)

    second = conv_second.reshape(9, channels, channels)
    first = jnp.transpose(conv_first, (0, 1, 3, 2)).reshape(9, latent, channels)
    w1, w2, wz, keep, rate = call(
        prep_kernel,
        tuple(
            in_hbm(x)
            for x in (first, second, time_weight, out_proj, keep_coef, noise_coef)
        ),
        [
            shape(channels, lanes(3 * slot), BF16), shape(FORMS, lanes(3 * channels) // 128, channels, 128, BF16),
            shape(4 * latent, 2 * channels, BF16),
            shape(*keep_coef.shape, F32), shape(*noise_coef.shape, F32),
        ],
        [pltpu.VMEM(x.shape, BF16) for x in (first, second, time_weight, out_proj)]
        + [pltpu.SemaphoreType.DMA((9,)), pltpu.SemaphoreType.DMA((5,))],
        4, 16, pl.BlockSpec(memory_space=pltpu.HBM),
    )
    weights = (w1, w2, wz)
    coefs = (keep, rate)
    around = (odd, own, even)

    def spare(row_tiles):
        return [pltpu.VMEM((SLOTS, FORMS, row_tiles, 3 * channels, width), BF16)]

    place = (dims, frames, levels, tiles)
    full, near, far = call(
        functools.partial(step0_kernel, *place),
        coefs + around + weights,
        [shape(flat + 2 * latent, n_wide, F32)] + [shape(2 * latent, n_wide, F32)] * 2,
        spare(rows // TILE + 1) + [pltpu.VMEM((frames, 4 * latent, n_wide), F32)],
        frames * (rows + 4), 32,
    )
    upd = swap(full, "level", levels, lambda d: (d + 2) % levels)
    far = swap(far, "level", levels, lambda d: (d - 1 if d % 2 == 0 else d + 1) % levels)
    near = swap(near, "level", levels, lambda d: d + 1 if d % 2 == 0 else d - 1)
    lat, zin = call(
        functools.partial(inner_kernel, *place),
        around + (upd,) + weights,
        [shape(frames - 2, latent, n_out, F32), shape(frames - 2, 4 * latent, n_out, F32)],
        spare(2 * rows // TILE), (frames - 2) * rows, 32,
    )
    (out,) = call(
        functools.partial(outer_kernel, *place),
        coefs + around + (upd, near, far, lat, zin) + weights,
        [shape(flat, rows, width, BF16)],
        spare(2 * rows // TILE) + [
            pltpu.VMEM((4, 4 * latent, n_out), F32), pltpu.VMEM((4, latent, n_out), F32),
        ],
        4 * rows, 32,
    )
    return out.reshape(1, frames, latent, rows, width)


def solution(mesh):
    return jax.shard_map(
        per_device,
        mesh=mesh,
        in_specs=(
            P("level", None, None, "tile", None),
            P(None, None, None, "tile", None),
            P(),
            P(),
            P(),
            P(),
            P(),
            P(),
        ),
        out_specs=P("level", None, None, "tile", None),
        check_vma=False,
    )
```

```python
import functools

import jax
import jax.numpy as jnp
from jax import lax
from jax.experimental import pallas as pl
from jax.experimental.pallas import tpu as pltpu
from jax.sharding import PartitionSpec as P

BF16 = jnp.bfloat16
F32 = jnp.float32
MIB = 1024 * 1024
AHEAD, SLOTS = 1, 2
TILE, FORMS = 4, 6


def dot(a, b):
    return jnp.dot(a, b, preferred_element_type=F32)


def slot_of(latent):
    return -(-3 * latent // 16) * 16


def lanes(n):
    return -(-n // 128) * 128


def prep_kernel(
    first_hbm, second_hbm, time_hbm, proj_hbm, keep_hbm, noise_hbm,
    w1_ref, w2_ref, wz_ref, keep_ref, noise_ref,
    first_ref, second_ref, time_ref, proj_ref, second_sem, sems,
):
    taps, latent, channels = first_hbm.shape
    slot = slot_of(latent)
    main = channels // 128 * 128
    loads = [
        pltpu.make_async_copy(src, dst, sems.at[k])
        for k, (src, dst) in enumerate(
            (
                (first_hbm, first_ref), (proj_hbm, proj_ref), (time_hbm, time_ref),
                (keep_hbm, keep_ref), (noise_hbm, noise_ref),
            )
        )
    ]
    slabs = [
        pltpu.make_async_copy(second_hbm.at[k], second_ref.at[k], second_sem.at[k])
        for k in range(taps)
    ]
    for b in range(3):
        for a in range(3):
            slabs[3 * a + b].start()
    for load in loads:
        load.start()
    full_blocks, tail = main // 128, channels - main
    blocks = w2_ref.shape[1]
    spare = blocks * 128 - 3 * channels
    if spare:
        w2_ref[:, blocks - 1, :, 128 - spare:] = jnp.zeros((FORMS, channels, spare), BF16)
    for b in range(3):
        for a in range(3):
            slabs[3 * a + b].wait()
        for lo in range(0, channels, 32):
            at = slice(lo, min(lo + 32, channels))
            g = [second_ref[3 * a + b, at].astype(F32) for a in range(3)]
            ends = g[0] + g[2]
            far_ends, middle = g[0] + 4.0 * g[2], 2.0 * g[1]
            forms = [
                0.125 * g[0], (1.0 / 12.0) * (ends + g[1]), (-1.0 / 24.0) * (ends - g[1]),
                (-1.0 / 48.0) * (far_ends + middle), (1.0 / 96.0) * (far_ends - middle),
                0.5 * g[2],
            ]
            for k, form in enumerate(forms):
                form = form.astype(BF16)
                for t in range(full_blocks):
                    w2_ref[k, b * full_blocks + t, at] = form[:, t * 128:(t + 1) * 128]
                start = 0
                while start < tail:
                    lane = b * tail + start
                    size = min(tail - start, 128 - lane % 128)
                    w2_ref[k, 3 * full_blocks + lane // 128, at, lane % 128:lane % 128 + size] = (
                        form[:, main + start:main + start + size]
                    )
                    start += size
    for load in loads:
        load.wait()
    pad = jnp.zeros((slot - 3 * latent, channels), F32)
    pieces = []
    for a in range(3):
        pieces += [first_ref[3 * a + b].astype(F32) for b in range(3)]
        if slot > 3 * latent:
            pieces.append(pad)
    w1 = 0.5 * jnp.concatenate(pieces, axis=0)
    w1 = jnp.pad(w1, ((0, w1_ref.shape[1] - 3 * slot), (0, lanes(channels) - channels)))
    w1_ref[...] = w1.T[0:channels].astype(BF16)
    proj = proj_ref[...]
    zero = jnp.zeros((latent, channels), F32)
    pt = [dot(proj, time_ref[k]) for k in range(3)]
    left = jnp.concatenate([2.0 * proj.astype(F32), zero, zero, zero], axis=0)
    right = jnp.concatenate([pt[1], pt[0], pt[2], zero], axis=0)
    wz_ref[:, 0:channels] = left.astype(BF16)
    wz_ref[:, channels:] = right.astype(BF16)


def row_forms(d):
    low = 4.0 * d[1]
    even1, odd1 = d[4] - 4.0 * d[2], d[3] - low
    even2, odd2 = d[4] - d[2], 2.0 * (d[3] - d[1])
    return (
        4.0 * d[0] + (even1 - d[2]), even1 + odd1, even1 - odd1, even2 + odd2, even2 - odd2,
        low + (d[5] - 5.0 * d[3]),
    )


def row_sums(product, put):
    n, h = product(1), 2.0 * product(2)
    even1, odd1 = n - h, n + h
    n, h = product(3), 2.0 * product(4)
    even2, odd2 = n - h, n + h
    put(1, -2.0 * odd2 - odd1)
    put(2, -4.0 * even2 - even1)
    put(0, (product(0) - even1) - even2)
    put(3, (product(5) - odd1) - 8.0 * odd2)


def gate(half):
    return half * jnp.tanh(half) + half


def convolve(batches, latents, dims, rows, tile, tiles, w1_ref, w2_ref, wz_ref, s_ref, store):
    latent, local_rows, width, channels = dims
    slot = slot_of(latent)
    parts_per = rows // TILE
    main = channels // 128 * 128
    extra = (rows - local_rows) // 2
    span = parts_per * width
    column = lax.broadcasted_iota(jnp.int32, (1, width), 1)
    not_first = jnp.where(column == 0, 0.0, 1.0)
    not_last = jnp.where(column == width - 1, 0.0, 1.0)
    top = jnp.where(tile == 0, 0.0, 1.0)
    bottom = jnp.where(tile == tiles - 1, 0.0, 1.0)

    def from_left(v):
        return pltpu.roll(v, 1, 1) * not_first.astype(v.dtype)

    def from_right(v):
        return pltpu.roll(v, width - 1, 1) * not_last.astype(v.dtype)

    def conv1(i, frames):
        for j, f in enumerate(frames):
            a = latents(f)
            b = []
            for r in range(rows + 4):
                v = a[:, r * width:(r + 1) * width]
                parts = [from_left(v), v, from_right(v)]
                if slot > 3 * latent:
                    parts.append(jnp.zeros((slot - 3 * latent, width), F32))
                b.append(jnp.concatenate(parts, axis=0))
            x = []
            for r in range(rows + 2):
                v = jnp.concatenate(b[r:r + 3], axis=0)
                if r <= extra:
                    v = v * top
                if r > extra + local_rows:
                    v = v * bottom
                x.append(v.astype(BF16))
            v = gate(dot(w1_ref[:, 0:3 * slot], jnp.concatenate(x, axis=1)))
            d = [v[:, r * width:(r + 1) * width] for r in range(rows + 2)]
            for p in range(parts_per):
                at = j * parts_per + p
                for k, form in enumerate(row_forms(d[TILE * p:TILE * p + FORMS])):
                    form = form.astype(BF16)
                    for c, v in enumerate((from_left(form), form, from_right(form))):
                        tail = 3 * main + c * (channels - main)
                        s_ref[i % SLOTS, k, at, c * main:(c + 1) * main, :] = v[0:main]
                        if main < channels:
                            s_ref[i % SLOTS, k, at, tail:tail + channels - main, :] = v[main:]

    def conv2(i, frames):
        def product(k):
            x = [s_ref[i % SLOTS, k, p] for p in range(len(frames) * parts_per)]
            w = jnp.concatenate([w2_ref[k, t] for t in range(w2_ref.shape[1])], axis=1)
            return dot(w[:, 0:3 * channels], jnp.concatenate(x, axis=1))

        ready = {}

        def put(r, half):
            ready[r] = jnp.concatenate([half.astype(BF16), gate(half).astype(BF16)], axis=0)

        row_sums(product, put)
        return ready

    def project(frames, ready):
        for r, x in ready.items():
            z = dot(wz_ref[...], x)
            for j, f in enumerate(frames):
                for p in range(parts_per):
                    at = (j * parts_per + p) * width
                    store(f, TILE * p + r, z[:, at:at + width])

    count = len(batches)
    for i in range(min(AHEAD, count)):
        conv1(i, batches[i])
    for i in range(count):
        if AHEAD == 1 and i + 1 < count:
            conv1(i + 1, batches[i + 1])
        ready = conv2(i, batches[i])
        if AHEAD == 2 and i + 2 < count:
            conv1(i + 2, batches[i + 2])
        project(batches[i], ready)


def narrow(v):
    return v.astype(BF16).astype(F32)


def neighbours(odd_ref, even_ref, tile, lo, hi):
    odd, even = odd_ref[lo:hi, :].astype(F32), even_ref[lo:hi, :].astype(F32)
    is_even = lax.rem(tile, 2) == 0
    return jnp.where(is_even, odd, even), jnp.where(is_even, even, odd)


def coef(ref, step, position, f):
    return ref[step, pl.ds(position, 1), f:f + 1]


def z_parts(z_ref, f, latent):
    return [z_ref[f, k * latent:(k + 1) * latent, :] for k in range(3)]


def step0_kernel(
    dims, frames, levels, tiles, keep_ref, noise_ref, odd_ref, own_ref, even_ref,
    w1_ref, w2_ref, wz_ref, full_ref, near_ref, far_ref, s_ref, z_ref,
):
    latent, local_rows, width, channels = dims
    rows = local_rows + 4
    level = lax.axis_index("level")
    position = lax.rem(level + 1, levels)
    even = lax.rem(level, 2) == 0
    flat = frames * latent
    tile = lax.axis_index("tile")

    def latents(f):
        lo, hi = f * latent, (f + 1) * latent
        prev, after = neighbours(odd_ref, even_ref, tile, lo, hi)
        own = own_ref[lo:hi, :].astype(F32)
        return jnp.concatenate(
            [prev[:, (local_rows - 4) * width:], own, after[:, 0:4 * width]], axis=1
        )

    def store(f, row, z):
        z_ref[f, :, row * width:(row + 1) * width] = z

    convolve(
        [(f,) for f in range(frames)], latents, dims, rows, tile, tiles,
        w1_ref, w2_ref, wz_ref, s_ref, store,
    )
    skip, updates = 2 * width, []
    for f in range(frames):
        z = z_parts(z_ref, f, latent)[0]
        if f > 0:
            z = z + z_parts(z_ref, f - 1, latent)[1]
        if f + 1 < frames:
            z = z + z_parts(z_ref, f + 1, latent)[2]
        lo, hi = f * latent, (f + 1) * latent
        q = latents(f)[:, skip:skip + rows * width]
        upd = coef(keep_ref, 0, position, f) * q - coef(noise_ref, 0, position, f) * z
        updates.append(upd)
    z_first, z_last = z_parts(z_ref, 0, latent)[2], z_parts(z_ref, frames - 1, latent)[1]
    first, last = updates[0], updates[-1]
    low_first, low_last = first - narrow(first), last - narrow(last)
    everything = updates + [z_last, z_first, low_first, low_last]
    full_ref[...] = jnp.concatenate(everything, axis=0).astype(BF16)
    backward = jnp.concatenate([z_first, first, low_first], axis=0)
    forward = jnp.concatenate([z_last, last, low_last], axis=0)
    near_ref[...] = jnp.where(even, backward, forward).astype(BF16)
    far_ref[...] = jnp.where(even, forward, backward).astype(BF16)


def window(f, dims, frames, tile, odd_ref, own_ref, even_ref):
    latent, local_rows, width, _ = dims
    lo, hi = (frames + f) * latent, (frames + f + 1) * latent
    prev, after = neighbours(odd_ref, even_ref, tile, lo, hi)
    own = own_ref[lo:hi, :].astype(F32)
    return jnp.concatenate(
        [prev[:, (local_rows - 2) * width:], own, after[:, 0:2 * width]], axis=1
    )


def inside(v, dims, tile, tiles):
    local_rows, width = dims[1], dims[2]
    row = lax.broadcasted_iota(jnp.int32, v.shape, 1) // width
    low = jnp.where(tile == 0, 2, 0)
    high = jnp.where(tile == tiles - 1, 2 + local_rows, local_rows + 4)
    return jnp.where((row < low) | (row >= high), 0.0, v).astype(BF16).astype(F32)


def inner_kernel(
    dims, frames, levels, tiles, odd_ref, own_ref, even_ref, upd_ref,
    w1_ref, w2_ref, wz_ref, lat_ref, zin_ref, s_ref,
):
    latent, local_rows, width, channels = dims
    level, tile = lax.axis_index("level"), lax.axis_index("tile")
    update = upd_ref[...].astype(F32)

    def latents(f):
        fresh = window(f, dims, frames, tile, odd_ref, own_ref, even_ref)
        v = jnp.where(level == 0, fresh, update[f * latent:(f + 1) * latent])
        v = inside(v, dims, tile, tiles)
        lat_ref[f - 1] = v[:, 2 * width:(2 + local_rows) * width]
        return v

    def store(f, row, z):
        zin_ref[f - 1, :, row * width:(row + 1) * width] = z

    inner = list(range(1, frames - 1))
    batches = [tuple(inner[k:k + 2]) for k in range(0, len(inner), 2)]
    convolve(
        batches, latents, dims, local_rows, tile, tiles, w1_ref, w2_ref, wz_ref, s_ref, store
    )


def outer_kernel(
    dims, frames, levels, tiles, keep_ref, noise_ref, odd_ref, own_ref, even_ref, upd_ref,
    near_ref, far_ref, lat_ref, zin_ref, w1_ref, w2_ref, wz_ref,
    out_ref, s_ref, z_ref, edge_ref,
):
    latent, local_rows, width, channels = dims
    level, tile = lax.axis_index("level"), lax.axis_index("tile")
    before = lax.rem(level + levels - 1, levels)
    last = frames - 1
    flat = frames * latent
    even = lax.rem(level, 2) == 0
    update = upd_ref[...].astype(F32)
    near, far = near_ref[...].astype(F32), far_ref[...].astype(F32)
    fwd_in, bwd_in = jnp.where(even, near, far), jnp.where(even, far, near)
    fwd, bwd, low_first, low_last = (
        update[flat + k * latent:flat + (k + 1) * latent] for k in range(4)
    )
    slots = {-1: 0, 0: 1, last: 2, frames: 3}

    def latents(f):
        source = last if f < 0 else min(f, last)
        fresh = window(source, dims, frames, tile, odd_ref, own_ref, even_ref)
        if f == -1:
            earlier = lax.rem(level + levels - 2, levels)
            v = fwd_in[latent:2 * latent] + fwd_in[2 * latent:] - coef(noise_ref, 0, earlier, last) * bwd
            v = jnp.where(level == 1, fresh, v)
            v = jnp.where(level == 0, 0.0, v)
        elif f == 0:
            rate = jnp.where(level == 1, 0.0, coef(noise_ref, 0, before, 0))
            v = update[0:latent] + low_first - rate * fwd_in[0:latent]
            v = jnp.where(level == 0, fresh, v)
        elif f == last:
            v = update[last * latent:flat] + low_last
            v = v - coef(noise_ref, 0, before, last) * bwd_in[0:latent]
            v = jnp.where(level == 0, fresh, v)
        else:
            rate = jnp.where(level == 0, 0.0, coef(noise_ref, 0, level, 0))
            v = bwd_in[latent:2 * latent] + bwd_in[2 * latent:] - rate * fwd
            v = jnp.where(level == levels - 1, 0.0, v)
        v = inside(v, dims, tile, tiles)
        edge_ref[slots[f]] = v[:, 2 * width:(2 + local_rows) * width]
        return v

    def store(f, row, z):
        z_ref[slots[f], :, row * width:(row + 1) * width] = z

    convolve(
        [(-1, 0), (last, frames)], latents, dims, local_rows, tile, tiles,
        w1_ref, w2_ref, wz_ref, s_ref, store,
    )

    def parts(f):
        if f in slots:
            return z_parts(z_ref, slots[f], latent)
        return z_parts(zin_ref, f - 1, latent)

    for f in range(frames):
        z = parts(f)[0] + parts(f - 1)[1] + parts(f + 1)[2]
        q = edge_ref[slots[f]] if f in slots else lat_ref[f - 1]
        out = coef(keep_ref, 1, level, f) * q - coef(noise_ref, 1, level, f) * z
        cut = [out[:, None, r * width:(r + 1) * width] for r in range(local_rows)]
        out_ref[f * latent:(f + 1) * latent] = jnp.concatenate(cut, axis=1).astype(BF16)


def per_device(
    queue_init, noise_frames, conv_first, conv_second, time_weight, out_proj, keep_coef, noise_coef
):
    steps = noise_frames.shape[0]
    _, frames, latent, rows, width = queue_init.shape
    channels = conv_second.shape[2]
    levels, tiles = lax.axis_size("level"), lax.axis_size("tile")
    level = lax.axis_index("level")
    assert steps == 2 and rows % TILE == 0 and levels % 4 == 0
    flat = frames * latent
    n_out, n_wide = rows * width, (rows + 4) * width
    dims = (latent, rows, width, channels)
    slot = slot_of(latent)

    vmem = pl.BlockSpec(memory_space=pltpu.VMEM)

    def shape(*dims_and_type):
        return jax.ShapeDtypeStruct(dims_and_type[:-1], dims_and_type[-1])

    def call(body, operands, outs, scratch, row_frames, grant, space=vmem):
        flops = 2 * row_frames * width * channels * 8 * channels
        return pl.pallas_call(
            body,
            out_shape=tuple(outs),
            in_specs=[space] * len(operands),
            out_specs=(vmem,) * len(outs),
            scratch_shapes=scratch,
            compiler_params=pltpu.CompilerParams(vmem_limit_bytes=grant * MIB),
            cost_estimate=pl.CostEstimate(
                flops=flops, bytes_accessed=channels * channels * 24, transcendentals=0
            ),
        )(*operands)

    def in_hbm(x):
        return pltpu.with_memory_space_constraint(x, pltpu.HBM)

    def swap(x, axis, size, partner):
        pairs = [(i, partner(i)) for i in range(size) if 0 <= partner(i) < size]
        return lax.ppermute(x, axis, pairs)

    queue = queue_init[0].reshape(flat, n_out)
    noise = noise_frames.reshape(steps, flat, n_out)
    pack = jnp.concatenate([jnp.where(level == levels - 1, noise[0], queue), noise[1]], axis=0)
    own = pack
    odd = swap(pack, "tile", tiles, lambda t: t - 1 if t % 2 == 0 else t + 1)
    even = swap(pack, "tile", tiles, lambda t: t + 1 if t % 2 == 0 else t - 1)

    second = conv_second.reshape(9, channels, channels)
    first = jnp.transpose(conv_first, (0, 1, 3, 2)).reshape(9, latent, channels)
    w1, w2, wz, keep, rate = call(
        prep_kernel,
        tuple(
            in_hbm(x)
            for x in (first, second, time_weight, out_proj, keep_coef, noise_coef)
        ),
        [
            shape(channels, lanes(3 * slot), BF16), shape(FORMS, lanes(3 * channels) // 128, channels, 128, BF16),
            shape(4 * latent, 2 * channels, BF16),
            shape(*keep_coef.shape, F32), shape(*noise_coef.shape, F32),
        ],
        [pltpu.VMEM(x.shape, BF16) for x in (first, second, time_weight, out_proj)]
        + [pltpu.SemaphoreType.DMA((9,)), pltpu.SemaphoreType.DMA((5,))],
        4, 16, pl.BlockSpec(memory_space=pltpu.HBM),
    )
    weights = (w1, w2, wz)
    coefs = (keep, rate)
    around = (odd, own, even)

    def spare(row_tiles):
        return [pltpu.VMEM((SLOTS, FORMS, row_tiles, 3 * channels, width), BF16)]

    place = (dims, frames, levels, tiles)
    full, near, far = call(
        functools.partial(step0_kernel, *place),
        coefs + around + weights,
        [shape(flat + 4 * latent, n_wide, BF16)] + [shape(3 * latent, n_wide, BF16)] * 2,
        spare(rows // TILE + 1) + [pltpu.VMEM((frames, 4 * latent, n_wide), F32)],
        frames * (rows + 4), 32,
    )
    upd = swap(full, "level", levels, lambda d: (d + 2) % levels)
    far = swap(far, "level", levels, lambda d: (d - 1 if d % 2 == 0 else d + 1) % levels)
    near = swap(near, "level", levels, lambda d: d + 1 if d % 2 == 0 else d - 1)
    lat, zin = call(
        functools.partial(inner_kernel, *place),
        around + (upd,) + weights,
        [shape(frames - 2, latent, n_out, F32), shape(frames - 2, 4 * latent, n_out, F32)],
        spare(2 * rows // TILE), (frames - 2) * rows, 32,
    )
    (out,) = call(
        functools.partial(outer_kernel, *place),
        coefs + around + (upd, near, far, lat, zin) + weights,
        [shape(flat, rows, width, BF16)],
        spare(2 * rows // TILE) + [
            pltpu.VMEM((4, 4 * latent, n_out), F32), pltpu.VMEM((4, latent, n_out), F32),
        ],
        4 * rows, 32,
    )
    return out.reshape(1, frames, latent, rows, width)


def solution(mesh):
    return jax.shard_map(
        per_device,
        mesh=mesh,
        in_specs=(
            P("level", None, None, "tile", None),
            P(None, None, None, "tile", None),
            P(),
            P(),
            P(),
            P(),
            P(),
            P(),
        ),
        out_specs=P("level", None, None, "tile", None),
        check_vma=False,
    )
```

```python
import functools

import jax
import jax.numpy as jnp
from jax import lax
from jax.experimental import pallas as pl
from jax.experimental.pallas import tpu as pltpu
from jax.sharding import PartitionSpec as P

BF16 = jnp.bfloat16
F32 = jnp.float32
MIB = 1024 * 1024
AHEAD, SLOTS = 1, 2
TILE, FORMS = 4, 6


def dot(a, b):
    return jnp.dot(a, b, preferred_element_type=F32)


def slot_of(latent):
    return -(-3 * latent // 16) * 16


def lanes(n):
    return -(-n // 128) * 128


def prep_kernel(
    first_hbm, second_hbm, time_hbm, proj_hbm, keep_hbm, noise_hbm,
    w1_ref, w2_ref, wz_ref, keep_ref, noise_ref,
    first_ref, second_ref, time_ref, proj_ref, second_sem, sems,
):
    taps, latent, channels = first_hbm.shape
    slot = slot_of(latent)
    main = channels // 128 * 128
    loads = [
        pltpu.make_async_copy(src, dst, sems.at[k])
        for k, (src, dst) in enumerate(
            (
                (first_hbm, first_ref), (proj_hbm, proj_ref), (time_hbm, time_ref),
                (keep_hbm, keep_ref), (noise_hbm, noise_ref),
            )
        )
    ]
    slabs = [
        pltpu.make_async_copy(second_hbm.at[k], second_ref.at[k], second_sem.at[k])
        for k in range(taps)
    ]
    for k in (0, 1, 3, 4):
        loads[k].start()
    for b in range(3):
        if b == 2:
            loads[2].start()
        for a in range(3):
            slabs[3 * a + b].start()
    full_blocks, tail = main // 128, channels - main
    blocks = w2_ref.shape[1]
    spare = blocks * 128 - 3 * channels
    if spare:
        w2_ref[:, blocks - 1, :, 128 - spare:] = jnp.zeros((FORMS, channels, spare), BF16)
    for k in (0, 1, 3, 4):
        loads[k].wait()
    pad = jnp.zeros((slot - 3 * latent, channels), F32)
    pieces = []
    for a in range(3):
        pieces += [first_ref[3 * a + b].astype(F32) for b in range(3)]
        if slot > 3 * latent:
            pieces.append(pad)
    w1 = 0.5 * jnp.concatenate(pieces, axis=0)
    w1 = jnp.pad(w1, ((0, w1_ref.shape[1] - 3 * slot), (0, lanes(channels) - channels)))
    w1_ref[...] = w1.T[0:channels].astype(BF16)
    for b in range(3):
        if b == 2:
            loads[2].wait()
            proj = proj_ref[...]
            zero = jnp.zeros((latent, channels), F32)
            pt = [dot(proj, time_ref[k]) for k in range(3)]
            left = jnp.concatenate([2.0 * proj.astype(F32), zero, zero, zero], axis=0)
            right = jnp.concatenate([pt[1], pt[0], pt[2], zero], axis=0)
            wz_ref[:, 0:channels] = left.astype(BF16)
            wz_ref[:, channels:] = right.astype(BF16)
        for a in range(3):
            slabs[3 * a + b].wait()
        for lo in range(0, channels, 32):
            at = slice(lo, min(lo + 32, channels))
            g = [second_ref[3 * a + b, at].astype(F32) for a in range(3)]
            ends = g[0] + g[2]
            far_ends, middle = g[0] + 4.0 * g[2], 2.0 * g[1]
            forms = [
                0.125 * g[0], (1.0 / 12.0) * (ends + g[1]), (-1.0 / 24.0) * (ends - g[1]),
                (-1.0 / 48.0) * (far_ends + middle), (1.0 / 96.0) * (far_ends - middle),
                0.5 * g[2],
            ]
            for k, form in enumerate(forms):
                form = form.astype(BF16)
                for t in range(full_blocks):
                    w2_ref[k, b * full_blocks + t, at] = form[:, t * 128:(t + 1) * 128]
                start = 0
                while start < tail:
                    lane = b * tail + start
                    size = min(tail - start, 128 - lane % 128)
                    w2_ref[k, 3 * full_blocks + lane // 128, at, lane % 128:lane % 128 + size] = (
                        form[:, main + start:main + start + size]
                    )
                    start += size


def row_forms(d):
    low = 4.0 * d[1]
    even1, odd1 = d[4] - 4.0 * d[2], d[3] - low
    even2, odd2 = d[4] - d[2], 2.0 * (d[3] - d[1])
    return (
        4.0 * d[0] + (even1 - d[2]), even1 + odd1, even1 - odd1, even2 + odd2, even2 - odd2,
        low + (d[5] - 5.0 * d[3]),
    )


def row_sums(product, put):
    n, h = product(1), 2.0 * product(2)
    even1, odd1 = n - h, n + h
    n, h = product(3), 2.0 * product(4)
    even2, odd2 = n - h, n + h
    put(1, -2.0 * odd2 - odd1)
    put(2, -4.0 * even2 - even1)
    put(0, (product(0) - even1) - even2)
    put(3, (product(5) - odd1) - 8.0 * odd2)


def gate(half):
    return half * jnp.tanh(half) + half


def convolve(batches, latents, dims, rows, tile, tiles, w1_ref, w2_ref, wz_ref, s_ref, store):
    latent, local_rows, width, channels = dims
    slot = slot_of(latent)
    parts_per = rows // TILE
    main = channels // 128 * 128
    extra = (rows - local_rows) // 2
    span = parts_per * width
    column = lax.broadcasted_iota(jnp.int32, (1, width), 1)
    not_first = jnp.where(column == 0, 0.0, 1.0)
    not_last = jnp.where(column == width - 1, 0.0, 1.0)
    top = jnp.where(tile == 0, 0.0, 1.0)
    bottom = jnp.where(tile == tiles - 1, 0.0, 1.0)

    def from_left(v):
        return pltpu.roll(v, 1, 1) * not_first.astype(v.dtype)

    def from_right(v):
        return pltpu.roll(v, width - 1, 1) * not_last.astype(v.dtype)

    def conv1(i, frames):
        for j, f in enumerate(frames):
            a = latents(f)
            b = []
            for r in range(rows + 4):
                v = a[:, r * width:(r + 1) * width]
                parts = [from_left(v), v, from_right(v)]
                if slot > 3 * latent:
                    parts.append(jnp.zeros((slot - 3 * latent, width), F32))
                b.append(jnp.concatenate(parts, axis=0))
            x = []
            for r in range(rows + 2):
                v = jnp.concatenate(b[r:r + 3], axis=0)
                if r <= extra:
                    v = v * top
                if r > extra + local_rows:
                    v = v * bottom
                x.append(v.astype(BF16))
            v = gate(dot(w1_ref[:, 0:3 * slot], jnp.concatenate(x, axis=1)))
            d = [v[:, r * width:(r + 1) * width] for r in range(rows + 2)]
            for p in range(parts_per):
                at = j * parts_per + p
                for k, form in enumerate(row_forms(d[TILE * p:TILE * p + FORMS])):
                    form = form.astype(BF16)
                    for c, v in enumerate((from_left(form), form, from_right(form))):
                        tail = 3 * main + c * (channels - main)
                        s_ref[i % SLOTS, k, at, c * main:(c + 1) * main, :] = v[0:main]
                        if main < channels:
                            s_ref[i % SLOTS, k, at, tail:tail + channels - main, :] = v[main:]

    def conv2(i, frames):
        def product(k):
            x = [s_ref[i % SLOTS, k, p] for p in range(len(frames) * parts_per)]
            w = jnp.concatenate([w2_ref[k, t] for t in range(w2_ref.shape[1])], axis=1)
            return dot(w[:, 0:3 * channels], jnp.concatenate(x, axis=1))

        ready = {}

        def put(r, half):
            ready[r] = jnp.concatenate([half.astype(BF16), gate(half).astype(BF16)], axis=0)

        row_sums(product, put)
        return ready

    def project(frames, ready):
        for r, x in ready.items():
            z = dot(wz_ref[...], x)
            for j, f in enumerate(frames):
                for p in range(parts_per):
                    at = (j * parts_per + p) * width
                    store(f, TILE * p + r, z[:, at:at + width])

    count = len(batches)
    for i in range(min(AHEAD, count)):
        conv1(i, batches[i])
    for i in range(count):
        if AHEAD == 1 and i + 1 < count:
            conv1(i + 1, batches[i + 1])
        ready = conv2(i, batches[i])
        if AHEAD == 2 and i + 2 < count:
            conv1(i + 2, batches[i + 2])
        project(batches[i], ready)


def narrow(v):
    return v.astype(BF16).astype(F32)


def neighbours(odd_ref, even_ref, tile, lo, hi):
    odd, even = odd_ref[lo:hi, :].astype(F32), even_ref[lo:hi, :].astype(F32)
    is_even = lax.rem(tile, 2) == 0
    return jnp.where(is_even, odd, even), jnp.where(is_even, even, odd)


def coef(ref, step, position, f):
    return ref[step, pl.ds(position, 1), f:f + 1]


def z_parts(z_ref, f, latent):
    return [z_ref[f, k * latent:(k + 1) * latent, :] for k in range(3)]


def step0_kernel(
    dims, frames, levels, tiles, keep_ref, noise_ref, odd_ref, own_ref, even_ref,
    w1_ref, w2_ref, wz_ref, full_ref, near_ref, far_ref, s_ref, z_ref,
):
    latent, local_rows, width, channels = dims
    rows = local_rows + 4
    level = lax.axis_index("level")
    position = lax.rem(level + 1, levels)
    even = lax.rem(level, 2) == 0
    flat = frames * latent
    tile = lax.axis_index("tile")

    def latents(f):
        lo, hi = f * latent, (f + 1) * latent
        prev, after = neighbours(odd_ref, even_ref, tile, lo, hi)
        own = own_ref[lo:hi, :].astype(F32)
        return jnp.concatenate(
            [prev[:, (local_rows - 4) * width:], own, after[:, 0:4 * width]], axis=1
        )

    def store(f, row, z):
        z_ref[f, :, row * width:(row + 1) * width] = z

    convolve(
        [(f,) for f in range(frames)], latents, dims, rows, tile, tiles,
        w1_ref, w2_ref, wz_ref, s_ref, store,
    )
    skip, updates = 2 * width, []
    for f in range(frames):
        z = z_parts(z_ref, f, latent)[0]
        if f > 0:
            z = z + z_parts(z_ref, f - 1, latent)[1]
        if f + 1 < frames:
            z = z + z_parts(z_ref, f + 1, latent)[2]
        lo, hi = f * latent, (f + 1) * latent
        q = latents(f)[:, skip:skip + rows * width]
        upd = coef(keep_ref, 0, position, f) * q - coef(noise_ref, 0, position, f) * z
        updates.append(upd)
    z_first, z_last = z_parts(z_ref, 0, latent)[2], z_parts(z_ref, frames - 1, latent)[1]
    first, last = updates[0], updates[-1]
    low_first, low_last = first - narrow(first), last - narrow(last)
    everything = updates + [z_last, z_first, low_first, low_last]
    full_ref[...] = jnp.concatenate(everything, axis=0).astype(BF16)
    backward = jnp.concatenate([z_first, first, low_first], axis=0)
    forward = jnp.concatenate([z_last, last, low_last], axis=0)
    near_ref[...] = jnp.where(even, backward, forward).astype(BF16)
    far_ref[...] = jnp.where(even, forward, backward).astype(BF16)


def window(f, dims, frames, tile, odd_ref, own_ref, even_ref):
    latent, local_rows, width, _ = dims
    lo, hi = (frames + f) * latent, (frames + f + 1) * latent
    prev, after = neighbours(odd_ref, even_ref, tile, lo, hi)
    own = own_ref[lo:hi, :].astype(F32)
    return jnp.concatenate(
        [prev[:, (local_rows - 2) * width:], own, after[:, 0:2 * width]], axis=1
    )


def inside(v, dims, tile, tiles):
    local_rows, width = dims[1], dims[2]
    row = lax.broadcasted_iota(jnp.int32, v.shape, 1) // width
    low = jnp.where(tile == 0, 2, 0)
    high = jnp.where(tile == tiles - 1, 2 + local_rows, local_rows + 4)
    return jnp.where((row < low) | (row >= high), 0.0, v).astype(BF16).astype(F32)


def inner_kernel(
    dims, frames, levels, tiles, odd_ref, own_ref, even_ref, upd_ref,
    w1_ref, w2_ref, wz_ref, lat_ref, zin_ref, s_ref,
):
    latent, local_rows, width, channels = dims
    level, tile = lax.axis_index("level"), lax.axis_index("tile")
    update = upd_ref[...].astype(F32)

    def latents(f):
        fresh = window(f, dims, frames, tile, odd_ref, own_ref, even_ref)
        v = jnp.where(level == 0, fresh, update[f * latent:(f + 1) * latent])
        v = inside(v, dims, tile, tiles)
        lat_ref[f - 1] = v[:, 2 * width:(2 + local_rows) * width]
        return v

    def store(f, row, z):
        zin_ref[f - 1, :, row * width:(row + 1) * width] = z

    inner = list(range(1, frames - 1))
    batches = [tuple(inner[k:k + 2]) for k in range(0, len(inner), 2)]
    convolve(
        batches, latents, dims, local_rows, tile, tiles, w1_ref, w2_ref, wz_ref, s_ref, store
    )


def outer_kernel(
    dims, frames, levels, tiles, keep_ref, noise_ref, odd_ref, own_ref, even_ref, upd_ref,
    near_ref, far_ref, lat_ref, zin_ref, w1_ref, w2_ref, wz_ref,
    out_ref, s_ref, z_ref, edge_ref,
):
    latent, local_rows, width, channels = dims
    level, tile = lax.axis_index("level"), lax.axis_index("tile")
    before = lax.rem(level + levels - 1, levels)
    last = frames - 1
    flat = frames * latent
    even = lax.rem(level, 2) == 0
    update = upd_ref[...].astype(F32)
    near, far = near_ref[...].astype(F32), far_ref[...].astype(F32)
    fwd_in, bwd_in = jnp.where(even, near, far), jnp.where(even, far, near)
    fwd, bwd, low_first, low_last = (
        update[flat + k * latent:flat + (k + 1) * latent] for k in range(4)
    )
    slots = {-1: 0, 0: 1, last: 2, frames: 3}

    def latents(f):
        source = last if f < 0 else min(f, last)
        fresh = window(source, dims, frames, tile, odd_ref, own_ref, even_ref)
        if f == -1:
            earlier = lax.rem(level + levels - 2, levels)
            v = fwd_in[latent:2 * latent] + fwd_in[2 * latent:] - coef(noise_ref, 0, earlier, last) * bwd
            v = jnp.where(level == 1, fresh, v)
            v = jnp.where(level == 0, 0.0, v)
        elif f == 0:
            rate = jnp.where(level == 1, 0.0, coef(noise_ref, 0, before, 0))
            v = update[0:latent] + low_first - rate * fwd_in[0:latent]
            v = jnp.where(level == 0, fresh, v)
        elif f == last:
            v = update[last * latent:flat] + low_last
            v = v - coef(noise_ref, 0, before, last) * bwd_in[0:latent]
            v = jnp.where(level == 0, fresh, v)
        else:
            rate = jnp.where(level == 0, 0.0, coef(noise_ref, 0, level, 0))
            v = bwd_in[latent:2 * latent] + bwd_in[2 * latent:] - rate * fwd
            v = jnp.where(level == levels - 1, 0.0, v)
        v = inside(v, dims, tile, tiles)
        edge_ref[slots[f]] = v[:, 2 * width:(2 + local_rows) * width]
        return v

    def store(f, row, z):
        z_ref[slots[f], :, row * width:(row + 1) * width] = z

    convolve(
        [(-1, 0), (last, frames)], latents, dims, local_rows, tile, tiles,
        w1_ref, w2_ref, wz_ref, s_ref, store,
    )

    def parts(f):
        if f in slots:
            return z_parts(z_ref, slots[f], latent)
        return z_parts(zin_ref, f - 1, latent)

    for f in range(frames):
        z = parts(f)[0] + parts(f - 1)[1] + parts(f + 1)[2]
        q = edge_ref[slots[f]] if f in slots else lat_ref[f - 1]
        out = coef(keep_ref, 1, level, f) * q - coef(noise_ref, 1, level, f) * z
        cut = [out[:, None, r * width:(r + 1) * width] for r in range(local_rows)]
        out_ref[f * latent:(f + 1) * latent] = jnp.concatenate(cut, axis=1).astype(BF16)


def per_device(
    queue_init, noise_frames, conv_first, conv_second, time_weight, out_proj, keep_coef, noise_coef
):
    steps = noise_frames.shape[0]
    _, frames, latent, rows, width = queue_init.shape
    channels = conv_second.shape[2]
    levels, tiles = lax.axis_size("level"), lax.axis_size("tile")
    level = lax.axis_index("level")
    assert steps == 2 and rows % TILE == 0 and levels % 4 == 0
    flat = frames * latent
    n_out, n_wide = rows * width, (rows + 4) * width
    dims = (latent, rows, width, channels)
    slot = slot_of(latent)

    vmem = pl.BlockSpec(memory_space=pltpu.VMEM)

    def shape(*dims_and_type):
        return jax.ShapeDtypeStruct(dims_and_type[:-1], dims_and_type[-1])

    def call(body, operands, outs, scratch, row_frames, grant, space=vmem):
        flops = 2 * row_frames * width * channels * 8 * channels
        return pl.pallas_call(
            body,
            out_shape=tuple(outs),
            in_specs=[space] * len(operands),
            out_specs=(vmem,) * len(outs),
            scratch_shapes=scratch,
            compiler_params=pltpu.CompilerParams(vmem_limit_bytes=grant * MIB),
            cost_estimate=pl.CostEstimate(
                flops=flops, bytes_accessed=channels * channels * 24, transcendentals=0
            ),
        )(*operands)

    def in_hbm(x):
        return pltpu.with_memory_space_constraint(x, pltpu.HBM)

    def swap(x, axis, size, partner):
        pairs = [(i, partner(i)) for i in range(size) if 0 <= partner(i) < size]
        return lax.ppermute(x, axis, pairs)

    queue = queue_init[0].reshape(flat, n_out)
    noise = noise_frames.reshape(steps, flat, n_out)
    pack = jnp.concatenate([jnp.where(level == levels - 1, noise[0], queue), noise[1]], axis=0)
    own = pack
    odd = swap(pack, "tile", tiles, lambda t: t - 1 if t % 2 == 0 else t + 1)
    even = swap(pack, "tile", tiles, lambda t: t + 1 if t % 2 == 0 else t - 1)

    second = conv_second.reshape(9, channels, channels)
    first = jnp.transpose(conv_first, (0, 1, 3, 2)).reshape(9, latent, channels)
    w1, w2, wz, keep, rate = call(
        prep_kernel,
        tuple(
            in_hbm(x)
            for x in (first, second, time_weight, out_proj, keep_coef, noise_coef)
        ),
        [
            shape(channels, lanes(3 * slot), BF16), shape(FORMS, lanes(3 * channels) // 128, channels, 128, BF16),
            shape(4 * latent, 2 * channels, BF16),
            shape(*keep_coef.shape, F32), shape(*noise_coef.shape, F32),
        ],
        [pltpu.VMEM(x.shape, BF16) for x in (first, second, time_weight, out_proj)]
        + [pltpu.SemaphoreType.DMA((9,)), pltpu.SemaphoreType.DMA((5,))],
        4, 16, pl.BlockSpec(memory_space=pltpu.HBM),
    )
    weights = (w1, w2, wz)
    coefs = (keep, rate)
    around = (odd, own, even)

    def spare(row_tiles):
        return [pltpu.VMEM((SLOTS, FORMS, row_tiles, 3 * channels, width), BF16)]

    place = (dims, frames, levels, tiles)
    full, near, far = call(
        functools.partial(step0_kernel, *place),
        coefs + around + weights,
        [shape(flat + 4 * latent, n_wide, BF16)] + [shape(3 * latent, n_wide, BF16)] * 2,
        spare(rows // TILE + 1) + [pltpu.VMEM((frames, 4 * latent, n_wide), F32)],
        frames * (rows + 4), 32,
    )
    upd = swap(full, "level", levels, lambda d: (d + 2) % levels)
    far = swap(far, "level", levels, lambda d: (d - 1 if d % 2 == 0 else d + 1) % levels)
    near = swap(near, "level", levels, lambda d: d + 1 if d % 2 == 0 else d - 1)
    lat, zin = call(
        functools.partial(inner_kernel, *place),
        around + (upd,) + weights,
        [shape(frames - 2, latent, n_out, F32), shape(frames - 2, 4 * latent, n_out, F32)],
        spare(2 * rows // TILE), (frames - 2) * rows, 32,
    )
    (out,) = call(
        functools.partial(outer_kernel, *place),
        coefs + around + (upd, near, far, lat, zin) + weights,
        [shape(flat, rows, width, BF16)],
        spare(2 * rows // TILE) + [
            pltpu.VMEM((4, 4 * latent, n_out), F32), pltpu.VMEM((4, latent, n_out), F32),
        ],
        4 * rows, 32,
    )
    return out.reshape(1, frames, latent, rows, width)


def solution(mesh):
    return jax.shard_map(
        per_device,
        mesh=mesh,
        in_specs=(
            P("level", None, None, "tile", None),
            P(None, None, None, "tile", None),
            P(),
            P(),
            P(),
            P(),
            P(),
            P(),
        ),
        out_specs=P("level", None, None, "tile", None),
        check_vma=False,
    )
```
